512 devices in a mesh: batch: 32 (over z, x), head: 16 (over y, core).
Axes of the slice: x: 4, y: 8, z: 8, core: 2. Of those that a mesh axis runs over, the one named last changes fastest.
Arguments:
- tokens: bfloat16 [16384, 2048], P('batch', 'head'), may hold values from -96 to 96
- lengths: int32 [128], P('batch'), may hold values from 1 to 128
- states: float32 [128, 16, 128, 128], P('batch', 'head'), may hold values from -3 to 3
- norm_gain: float32 [2048], replicated, may hold values from 0.1 to 1.9
- mix_weight: bfloat16 [2048, 14336], P(None, 'head'), may hold values from -0.125 to 0.125
- rate_weight: bfloat16 [2048, 64], P(None, 'head'), may hold values from -0.5524272 to 0.5524272
- decay_rate: float32 [16], P('head'), may hold values from 0.0005 to 0.03
- head_gain: float32 [128], replicated, may hold values from 0.1 to 1.9
- out_weight: bfloat16 [2048, 2048], P('head'), may hold values from -0.125 to 0.125
- final_gain: float32 [2048], replicated, may hold values from 0.1 to 1.9
- vocab_table: bfloat16 [16384, 2048], P(('batch', 'head')), may hold values from -50.8233 to 50.8233
- next_token: int32 [128], replicated, may hold values from 0 to 16383
Outputs:
- mixed: bfloat16 [16384, 2048], P('batch', 'head')
- new_state: float32 [128, 16, 128, 128], P('batch', 'head')
- log_likelihood: float32 [128], replicated
The draws below stay inside these ranges and needn't reach their ends.
All inputs are finite; a program needn't handle non-finite values.
Results may differ from the reference program's by a relative error of at most 0.0058.
The reference program's roundings to bfloat16 on the way count: a program that leaves them out, or rounds other values in their place, can miss the bound.
Values may be sent and summed in bfloat16 or wider, within the bound.
A program may use at most 64 MiB of HBM per device.

```python
import math
import jax
import jax.numpy as jnp
import numpy as np
from jax import lax

D = 2048
HEADS = 16
HEAD_DIM = 128
REFLECT = 3
VOCAB = 16384
NEW_POSITIONS = 128
SEQUENCE_COUNT = 128
TOKEN_ROWS_ALL = 16384


def householder_directions(key):
    reflect_vectors = jnp.clip(jax.random.normal(jax.random.fold_in(key, 101), (D, HEADS), jnp.float32), -4.0, 4.0)
    return reflect_vectors / jnp.sqrt(1.0 * D)


def draw_tokens(key, part):
    reflect_vectors = householder_directions(key)
    shared_way = jnp.sum(reflect_vectors, axis=1)
    shared_way = shared_way / jnp.sqrt(jnp.sum(shared_way * shared_way))
    column_scale = 0.3 * 10.0 ** (jnp.arange(D, dtype=jnp.float32) / (D - 1))
    row_scale = 10.0 ** jax.random.uniform(jax.random.fold_in(key, 102), (TOKEN_ROWS_ALL, 1), jnp.float32, -1.0, 0.0)
    base = jnp.clip(jax.random.normal(jax.random.fold_in(key, 103), (TOKEN_ROWS_ALL, D), jnp.float32), -4.0, 4.0)
    values = base * row_scale * column_scale
    householder_steps = jax.random.randint(jax.random.fold_in(key, 105), (SEQUENCE_COUNT, 2), 0, NEW_POSITIONS)
    position_places = jnp.arange(NEW_POSITIONS)
    masked_entries = jnp.any(position_places[None, :, None] == householder_steps[:, None, :], axis=2).reshape(TOKEN_ROWS_ALL, 1)
    values = values + jnp.where(masked_entries, 80.0 * shared_way[None, :], 0.0)
    return values.astype(jnp.bfloat16)


def draw_rate_weight(key, part):
    reflect_vectors = householder_directions(key)
    noise = jnp.clip(jax.random.normal(jax.random.fold_in(key, 111), (D, HEADS, REFLECT + 1), jnp.float32), -5.0, 5.0)
    noise = noise / jnp.sqrt(1.0 * D)
    boost = jnp.concatenate([jnp.zeros((D, HEADS, REFLECT), jnp.float32), 5.0 * reflect_vectors[:, :, None]], axis=2)
    return (noise + boost).reshape(D, HEADS * (REFLECT + 1)).astype(jnp.bfloat16)


def draw_decay_rate(key, part):
    spread = jax.random.uniform(jax.random.fold_in(key, 121), (HEADS,), jnp.float32)
    rates = 0.002 * 15.0 ** spread
    return rates


def draw_vocab_table(key, part):
    row_scale = 10.0 ** jax.random.uniform(jax.random.fold_in(key, 131), (VOCAB, 1), jnp.float32)
    base = jnp.clip(jax.random.normal(jax.random.fold_in(key, 132), (VOCAB, D), jnp.float32), -5.0, 5.0)
    values = base * row_scale / jnp.sqrt(1.0 * D)
    return values.astype(jnp.bfloat16)


def touch_ends(values, own_key, least, high):
    extent = values.shape
    index_at = [jax.random.randint(jax.random.fold_in(own_key, axis), (), 0, extent[axis]) for axis in range(len(extent))]
    values = values.at[tuple(index_at)].set(least)
    longest = extent.index(max(extent))
    index_at[longest] = (index_at[longest] + 1) % extent[longest]
    return values.at[tuple(index_at)].set(high)


def level_of(own_key, dims, split, smallest, top_value):
    gain, own = 1.0, jax.random.fold_in(own_key, 6)
    for axis_at, blocks in split:
        heights = jnp.exp(jax.random.uniform(jax.random.fold_in(own, axis_at), (blocks,), jnp.float32, smallest / len(split), top_value / len(split)))
        gain = gain * jnp.repeat(heights, dims[axis_at] // blocks).reshape([-1 if axis == axis_at else 1 for axis in range(len(dims))])
    return gain


def rank_bounds(amount, slope):
    loads = [(1 << 20) // math.isqrt(rank ** slope) + 1 for rank in range(1, amount + 1)]
    scale = 1 + sum(loads) // (1 << 30)
    return np.cumsum(np.array([max(1, weight // scale) for weight in loads]))


def ranked(key, shape, number_of, slope):
    table = rank_bounds(number_of, slope)
    ticket = jax.random.randint(jax.random.fold_in(key, 1), shape, 0, int(table[number_of - 1]))
    standing = jnp.searchsorted(jnp.asarray(table, jnp.int32), ticket, side="right")
    return jax.random.permutation(jax.random.fold_in(key, 2), number_of)[standing].astype(jnp.int32)


def bell_draw(stream_key, shape, scale, most, cuts=(), kind=jnp.bfloat16):
    drawn = jax.random.normal(stream_key, shape, jnp.float32) * scale
    if len(cuts) > 0:
        drawn = level_of(stream_key, shape, cuts, -0.22, 0.18) * drawn
    return jnp.clip(drawn, min=-most, max=most).astype(kind)


def setup_inputs(seed: int = 0) -> dict:
    streams_of = jax.random.split(jax.random.key(seed), 13)
    tokens = draw_tokens(jax.random.fold_in(streams_of[12], 71), 0)
    lengths = touch_ends(jax.random.randint(streams_of[1], (SEQUENCE_COUNT,), 1, NEW_POSITIONS + 1), jax.random.fold_in(streams_of[1], 1), 1, NEW_POSITIONS).astype(jnp.int32)
    states = bell_draw(streams_of[2], (SEQUENCE_COUNT, HEADS, HEAD_DIM, HEAD_DIM), 0.5, 3.0, ((0, 32), (1, 16)), jnp.float32)
    norm_gain = jnp.clip(1.0 + 0.18 * jax.random.normal(streams_of[3], (D,), jnp.float32), 0.1, 1.9)
    mix_weight = bell_draw(streams_of[4], (D, HEADS * (2 * REFLECT + 1) * HEAD_DIM), D ** -0.5, 0.125, ((1, 16),))
    rate_weight = draw_rate_weight(jax.random.fold_in(streams_of[12], 71), 0)
    decay_rate = draw_decay_rate(jax.random.fold_in(streams_of[12], 71), 0)
    head_gain = jnp.clip(1.0 + 0.18 * jax.random.normal(streams_of[7], (HEAD_DIM,), jnp.float32), 0.1, 1.9)
    out_weight = bell_draw(streams_of[8], (HEADS * HEAD_DIM, D), (HEADS * HEAD_DIM) ** -0.5, 0.125, ((0, 16),))
    final_gain = jnp.clip(1.0 + 0.18 * jax.random.normal(streams_of[9], (D,), jnp.float32), 0.1, 1.9)
    vocab_table = draw_vocab_table(jax.random.fold_in(streams_of[12], 71), 0)
    next_token = touch_ends(ranked(streams_of[11], (SEQUENCE_COUNT,), VOCAB, 2), jax.random.fold_in(streams_of[11], 3), 0, VOCAB - 1).astype(jnp.int32)
    return dict(tokens=tokens, lengths=lengths, states=states, norm_gain=norm_gain, mix_weight=mix_weight, rate_weight=rate_weight, decay_rate=decay_rate, head_gain=head_gain, out_weight=out_weight, final_gain=final_gain, vocab_table=vocab_table, next_token=next_token)


ROW_EPSILON = 1e-05
KEY_EPSILON = 1e-06
HIGHEST_PRECISION = lax.Precision.HIGHEST

def delta_block(queries, key_rows, value_rows, beta_rows, log_decay, start_state):
    positions = key_rows.shape[0]
    reflections = key_rows.shape[1]
    total_steps = positions * reflections
    flat_keys = key_rows.reshape(total_steps, key_rows.shape[2])
    flat_values = value_rows.reshape(total_steps, value_rows.shape[2])
    flat_betas = beta_rows.reshape(total_steps)
    padding = jnp.zeros((positions, reflections - 1), log_decay.dtype)
    step_decay = jnp.concatenate([log_decay[:, None], padding], axis=1).reshape(total_steps)
    cumulative = jnp.cumsum(step_decay)
    step_index = jnp.arange(total_steps)
    earlier = step_index[:, None] > step_index[None, :]
    decay_ratio = jnp.exp(jnp.where(earlier, cumulative[:, None] - cumulative[None, :], -jnp.inf))
    key_gram = jnp.dot(flat_keys, flat_keys.T, precision=HIGHEST_PRECISION)
    system = jnp.eye(total_steps, dtype=key_gram.dtype) + flat_betas[:, None] * decay_ratio * key_gram
    start_image = jnp.dot(flat_keys, start_state.T, precision=HIGHEST_PRECISION)
    source = flat_betas[:, None] * (flat_values - jnp.exp(cumulative)[:, None] * start_image)
    updates = jax.scipy.linalg.solve_triangular(system, source, lower=True, unit_diagonal=True)
    query_cumulative = cumulative.reshape(positions, reflections)[:, reflections - 1]
    query_step = step_index.reshape(positions, reflections)[:, reflections - 1]
    visible = step_index[None, :] <= query_step[:, None]
    weights = jnp.exp(jnp.where(visible, query_cumulative[:, None] - cumulative[None, :], -jnp.inf))
    scores = jnp.dot(queries, flat_keys.T, precision=HIGHEST_PRECISION) * weights
    attended = jnp.exp(query_cumulative)[:, None] * jnp.dot(queries, start_state.T, precision=HIGHEST_PRECISION)
    attended = attended + jnp.dot(scores, updates, precision=HIGHEST_PRECISION)
    tail_decay = jnp.exp(cumulative[total_steps - 1] - cumulative)
    new_state = jnp.exp(cumulative[total_steps - 1]) * start_state
    new_state = new_state + jnp.dot(updates.T, tail_decay[:, None] * flat_keys, precision=HIGHEST_PRECISION)
    return (attended, new_state)

def head_inputs(projected, rate_logits, valid_mask, decay_rate):
    queries = jax.nn.silu(projected[:, :, :, 0])
    key_rows = jax.nn.silu(projected[:, :, :, 1:REFLECT + 1])
    key_rows = key_rows * lax.rsqrt(lax.optimization_barrier(jnp.sum(key_rows * key_rows, axis=-1, keepdims=True)) + KEY_EPSILON)
    value_rows = jax.nn.silu(projected[:, :, :, REFLECT + 1:])
    beta_rows = jnp.where(valid_mask[:, :, None, None], 2.0 * jax.nn.sigmoid(rate_logits[..., :REFLECT]), 0.0)
    log_decay = jnp.where(valid_mask[:, :, None], -decay_rate * jax.nn.softplus(rate_logits[..., REFLECT]), 0.0)
    return (queries, key_rows, value_rows, beta_rows, log_decay)

def run_heads(queries, key_rows, value_rows, beta_rows, log_decay, start_states):
    per_head = jax.vmap(delta_block, in_axes=(1, 1, 1, 1, 1, 0), out_axes=(1, 0))
    per_sequence = jax.vmap(per_head)
    return per_sequence(queries, key_rows, value_rows, beta_rows, log_decay, start_states)

def head_norm(attended, head_gain):
    factor = lax.rsqrt(lax.optimization_barrier(jnp.mean(attended * attended, axis=-1, keepdims=True)) + ROW_EPSILON)
    return (attended * factor * head_gain).astype(jnp.bfloat16)

def reference(tokens, lengths, states, norm_gain, mix_weight, rate_weight, decay_rate, head_gain, out_weight, final_gain, vocab_table, next_token):
    model_width = tokens.shape[1]
    blocks = tokens.reshape(lengths.shape[0], NEW_POSITIONS, model_width)

    def one_sequence(inputs):
        block_rows, length, start_state = inputs
        widened = block_rows.astype(jnp.float32)
        scaled = (widened * norm_gain).astype(jnp.bfloat16)
        inverse = lax.rsqrt(lax.optimization_barrier(jnp.mean(widened * widened, axis=1, keepdims=True)) + ROW_EPSILON)
        projected = jnp.dot(scaled.astype(jnp.float32), mix_weight.astype(jnp.float32), preferred_element_type=jnp.float32) * inverse
        rate_logits = jnp.dot(scaled.astype(jnp.float32), rate_weight.astype(jnp.float32), preferred_element_type=jnp.float32) * inverse
        projected = projected.reshape(1, NEW_POSITIONS, HEADS, 2 * REFLECT + 1, HEAD_DIM)
        rate_logits = rate_logits.reshape(1, NEW_POSITIONS, HEADS, REFLECT + 1)
        valid_mask = (jnp.arange(NEW_POSITIONS) < length)[None, :]
        queries, key_rows, value_rows, beta_rows, log_decay = head_inputs(projected, rate_logits, valid_mask, decay_rate)
        attended, new_state = run_heads(queries, key_rows, value_rows, beta_rows, log_decay, start_state[None])
        normed = head_norm(attended, head_gain).reshape(NEW_POSITIONS, HEADS * HEAD_DIM)
        mixed = (widened + jnp.dot(normed.astype(jnp.float32), out_weight.astype(jnp.float32), preferred_element_type=jnp.float32)).astype(jnp.bfloat16)
        last_row = lax.dynamic_slice_in_dim(mixed, (length - 1).astype(jnp.int32), 1, 0)[0]
        return (mixed, new_state[0], last_row)
    mixed, new_state, last_rows = lax.map(one_sequence, (blocks, lengths, states))
    widened = last_rows.astype(jnp.float32)
    factor = lax.rsqrt(lax.optimization_barrier(jnp.mean(widened * widened, axis=1, keepdims=True)) + ROW_EPSILON)
    hidden = (widened * factor * final_gain).astype(jnp.bfloat16)
    logits = jnp.dot(hidden.astype(jnp.float32), vocab_table.T.astype(jnp.float32), preferred_element_type=jnp.float32)
    largest = lax.optimization_barrier(jnp.max(logits, axis=1))
    exp_total = lax.optimization_barrier(jnp.sum(jnp.exp(logits - largest[:, None]), axis=1))
    target = jnp.take_along_axis(logits, next_token[:, None], axis=1)[:, 0]
    log_likelihood = target - (largest + jnp.log(exp_total))
    return (mixed.reshape(tokens.shape), new_state, log_likelihood)
```

```python
import jax
import jax.numpy as jnp
from jax import lax
from jax.experimental import pallas as pl
from jax.experimental.pallas import tpu as pltpu
from jax.sharding import Mesh
from jax.sharding import PartitionSpec as P

HEAD_DIM = 128
REFLECT = 3
NEW_POSITIONS = 128
HEAD = ("head_0", "head_1")
BATCH_HEAD = ("batch_0", "batch_1", "head_0", "head_1")
BATCH = ("batch_0", "batch_1")
BF = jnp.bfloat16
F32 = jnp.float32
HI = lax.Precision.HIGHEST
N = 128
CH = 32
NC = N // CH
LEVELS = 7
ROW_EPSILON = 1e-05
KEY_EPSILON = 1e-06


def split(x):
    high = x.astype(BF)
    return high, (x - high.astype(F32)).astype(BF)


def left_of(x):
    high, low = split(x)
    return jnp.concatenate([high, low], axis=1)


def right_of(x):
    high, low = split(x)
    both = jnp.concatenate([high, low], axis=1)
    return jnp.concatenate([both, both], axis=0)


def halves(product):
    return product[:, :N] + product[:, N:]


def dot(a, b):
    return jnp.dot(a, b, preferred_element_type=F32)


def dot_nt(a, b):
    return lax.dot_general(a, b, (((1,), (1,)), ((), ())), preferred_element_type=F32)


def fill_tables(masks, tri, picks):
    row = lax.broadcasted_iota(jnp.int32, (N, N), 0)
    col = lax.broadcasted_iota(jnp.int32, (N, N), 1)
    j, p, jj, pp = row // CH, row % CH, col // CH, col % CH
    steps = (j < 3) & (jj < 3)
    sets = [steps & (p == pp) & (j == 1) & (jj == 0), steps & (p == pp) & (j == 2) & (jj < 2)]
    for k in range(5):
        same = (p >> (k + 1)) == (pp >> (k + 1))
        sets.append(steps & same & (((p >> k) & 1) == 1) & (((pp >> k) & 1) == 0))
    sets.append((j == 3) & (jj < 3))
    for k, chosen in enumerate(sets):
        masks[k] = chosen.astype(F32)
    strict = steps & ((p > pp) | ((p == pp) & (j > jj)))
    masks[LEVELS + 1] = (strict | ((j == 3) & (jj < 3) & (p >= pp))).astype(F32)
    tri[...] = ((j == jj) & (pp <= p)).astype(F32)
    for c in range(NC):
        picks[:, c * N : (c + 1) * N] = ((j == c) & (p <= pp)).astype(F32)


def silu(v):
    return v / (1.0 + jnp.exp(-v))


def softplus(v):
    return jnp.maximum(v, 0.0) + jnp.log1p(jnp.exp(-jnp.abs(v)))


def sequence_inputs(s, length, rate, blocks, gain, weight, rate_t, masks, tri, picks, xs, la, tt, xh, xl, kt, eq, et):
    count = blocks.shape[0]
    rows = pl.ds(pl.multiple_of(s * N, N), N)
    squares = jnp.zeros((N, N), F32)
    for b in range(count):
        wide = blocks[b, rows, :].astype(F32)
        squares = squares + wide * wide
        xs[:, b * N : (b + 1) * N] = (wide * gain[b : b + 1, :]).astype(BF)
    inverse = lax.rsqrt(jnp.sum(squares, axis=1, keepdims=True) / (count * N) + ROW_EPSILON)
    projected = dot(xs[...], weight[...]) * inverse
    rates = dot_nt(xs[...], rate_t[...]) * inverse
    query = silu(projected[:, :N])
    keys, values = [], []
    for j in range(3):
        key = silu(projected[:, (1 + j) * N : (2 + j) * N])
        keys.append(key * lax.rsqrt(jnp.sum(key * key, axis=1, keepdims=True) + KEY_EPSILON))
        values.append(silu(projected[:, (4 + j) * N : (5 + j) * N]))
    valid = lax.broadcasted_iota(jnp.int32, (N, 1), 0) < length
    betas = [
        jnp.broadcast_to(jnp.where(valid, 2.0 * jax.nn.sigmoid(rates[:, j : j + 1]), 0.0), (N, N))
        for j in range(3)
    ]
    decay = jnp.where(valid, -rate * softplus(rates[:, 3:4]), 0.0)
    decay = jnp.broadcast_to(decay, (N, N))
    cum = jnp.dot(tri[...], decay, precision=HI, preferred_element_type=F32)
    cum_row = jnp.dot(decay.T[:8], picks[...], precision=HI, preferred_element_type=F32)
    grow = jnp.exp(cum)
    one = jnp.ones((CH, N), F32)
    zero = jnp.zeros((CH, N), F32)
    eye = (
        lax.broadcasted_iota(jnp.int32, (N, N), 0) == lax.broadcasted_iota(jnp.int32, (N, N), 1)
    ).astype(F32)
    causal = masks[LEVELS + 1] > 0.5
    first = masks[0]
    for c in range(NC):
        at = slice(c * CH, (c + 1) * CH)
        n = s * NC + c
        kq = jnp.concatenate([keys[0][at], keys[1][at], keys[2][at], query[at]], axis=0)
        vv = jnp.concatenate([values[0][at], values[1][at], values[2][at], zero], axis=0)
        bb = jnp.concatenate([betas[0][at], betas[1][at], betas[2][at], one], axis=0)
        cc = jnp.concatenate([cum[at]] * 4, axis=0)
        gg = jnp.concatenate([grow[at]] * 3 + [zero], axis=0)
        high, low = split(kq)
        gram = halves(
            dot_nt(
                jnp.concatenate([high, low], axis=1),
                jnp.concatenate(
                    [jnp.concatenate([high, high], axis=1), jnp.concatenate([low, low], axis=1)],
                    axis=0,
                ),
            )
        )
        ratio = jnp.exp(jnp.where(causal, cc - cum_row[0:1, c * N : (c + 1) * N], -1e30))
        system = bb * ratio * gram
        la[n] = system
        tt[n] = eye - system * first
        xa, xb = bb * vv, bb * gg * kq
        ha, lo_a = split(xa)
        hb, lo_b = split(xb)
        xh[n] = jnp.concatenate([ha, hb], axis=1)
        xl[n] = jnp.concatenate([lo_a, lo_b], axis=1)
        last = cum[(c + 1) * CH - 1 : (c + 1) * CH, :]
        tail = jnp.concatenate([jnp.exp(last - cum[at])] * 3 + [zero], axis=0)
        kt[n] = left_of((tail * kq).T)
        eq[n] = grow[at] * query[at]
        et[n] = jnp.broadcast_to(jnp.exp(last), (8, N))


def invert(ids, masks, la, tt, tmp):
    def level(k, carry):
        mask = masks[k]
        for n in ids:
            tmp[n] = halves(dot(left_of(la[n] * mask), right_of(tt[n])))
        for n in ids:
            t = tt[n]
            tt[n] = t - halves(dot(left_of(t), right_of(tmp[n])))
        return carry

    lax.fori_loop(1, LEVELS + 1, level, 0)


def chunk_maps(n, tt, xh, xl, kt, eq, et, pq, rr, ov):
    high, low = split(tt[n])
    big = jnp.concatenate([high, low], axis=1)
    z = dot(big, jnp.concatenate([xh[n], xh[n]], axis=0)) + dot(high, xl[n])
    zh, zl = split(z)
    k = kt[n]
    maps = dot(k, jnp.concatenate([zh, zh], axis=0)) + dot(k[:, :N], zl)
    eye = (
        lax.broadcasted_iota(jnp.int32, (N, N), 0) == lax.broadcasted_iota(jnp.int32, (N, N), 1)
    ).astype(F32)
    p = eye * et[n, 0:1, :] - maps[:, N:]
    pq[n] = left_of(jnp.concatenate([p, eq[n] + z[3 * CH :, N:]], axis=0))
    rr[n] = maps[:, :N]
    ov[n] = -z[3 * CH :, :N]


def run_chain(sequences, states, new_state, normed, head_gain, pq, rr, ov):
    carried = [states[s].T for s in sequences]
    for c in range(NC):
        for k, s in enumerate(sequences):
            n = s * NC + c
            both = halves(dot(pq[n], right_of(carried[k])))
            carried[k] = both[:N] + rr[n]
            attended = both[N:] + ov[n]
            factor = lax.rsqrt(jnp.mean(attended * attended, axis=1, keepdims=True) + ROW_EPSILON)
            normed[s * N + c * CH : s * N + (c + 1) * CH, :] = (
                attended * factor * head_gain[...]
            ).astype(BF)
    for k, s in enumerate(sequences):
        new_state[s] = carried[k].T


def mixer_scratch(seqs, count, width):
    m = seqs * NC
    return [
        pltpu.VMEM((LEVELS + 2, N, N), F32),
        pltpu.VMEM((N, N), F32),
        pltpu.VMEM((N, NC * N), F32),
        pltpu.VMEM((N, count * N), BF),
        pltpu.VMEM((m, N, N), F32),
        pltpu.VMEM((m, N, N), F32),
        pltpu.VMEM((m, N, N), F32),
        pltpu.VMEM((m, N, 2 * N), BF),
        pltpu.VMEM((m, N, 2 * N), BF),
        pltpu.VMEM((m, N, 2 * N), BF),
        pltpu.VMEM((m, CH, N), F32),
        pltpu.VMEM((m, 8, N), F32),
        pltpu.VMEM((m, N + CH, 2 * N), BF),
        pltpu.VMEM((m, N, N), F32),
        pltpu.VMEM((m, CH, N), F32),
    ]


def mixer_kernel(lengths, rate, blocks, gain, weight, rate_t, head_gain, states, normed, new_state, masks, tri, picks, xs, la, tt, tmp, xh, xl, kt, eq, et, pq, rr, ov):
    seqs = states.shape[0]
    fill_tables(masks, tri, picks)

    def one(s, carry):
        sequence_inputs(s, lengths[s], rate[0], blocks, gain, weight, rate_t, masks, tri, picks, xs, la, tt, xh, xl, kt, eq, et)
        return carry

    lax.fori_loop(0, seqs, one, 0)
    invert(range(seqs * NC), masks, la, tt, tmp)

    def maps(s, carry):
        for c in range(NC):
            chunk_maps(s * NC + c, tt, xh, xl, kt, eq, et, pq, rr, ov)
        return carry

    lax.fori_loop(0, seqs, maps, 0)
    run_chain(range(seqs), states, new_state, normed, head_gain, pq, rr, ov)


def mixer(lengths, rate, blocks, gain, weight, rate_t, head_gain, states):
    seqs, rows, count = states.shape[0], blocks.shape[1], blocks.shape[0]
    vmem = pl.BlockSpec(memory_space=pltpu.VMEM)
    smem = pl.BlockSpec(memory_space=pltpu.SMEM)
    return pl.pallas_call(
        mixer_kernel,
        out_shape=(
            jax.ShapeDtypeStruct((rows, N), BF),
            jax.ShapeDtypeStruct((seqs, N, N), F32),
        ),
        in_specs=[smem, smem] + [vmem] * 6,
        out_specs=(vmem, vmem),
        scratch_shapes=mixer_scratch(seqs, count, weight.shape[1]),
        compiler_params=pltpu.CompilerParams(vmem_limit_bytes=56 * 1024 * 1024),
    )(lengths, rate, blocks, gain, weight, rate_t, head_gain, states)


def all_in_one(array, axis):
    leaves = jax.tree.leaves(array)
    order = sorted(range(len(leaves)), key=lambda k: -leaves[k].size)
    width = (1, *leaves[order[0]].shape)[-1]
    lines = [
        jnp.pad(leaves[k].reshape(-1), (0, -leaves[k].size % width)).reshape(-1, width)
        for k in order
    ]
    both, at, found = (lax.all_gather(jnp.concatenate(lines), axis), 0, {})
    for k, line in zip(order, lines):
        share = both[:, at : at + len(line)].reshape(len(both), -1)
        found[k] = share[:, : leaves[k].size].reshape(-1, *leaves[k].shape)
        at += len(line)
    numbers = iter(range(len(leaves)))
    return jax.tree.map(lambda _: found[next(numbers)], array)


def joined_all(array, axes, combine):
    for axis in axes:
        pieces = all_in_one(array, axis)
        array = jax.tree.map(lambda part: part[0], pieces)
        for k in range(1, lax.axis_size(axis)):
            array = combine(array, jax.tree.map(lambda part: part[k], pieces))
    return array


def combine_totals(earlier_part, later_part):
    highest = jnp.maximum(earlier_part[0], later_part[0])
    summed = earlier_part[1] * jnp.exp(earlier_part[0] - highest) + later_part[1] * jnp.exp(
        later_part[0] - highest
    )
    return (highest, summed, earlier_part[2] + later_part[2])


def on_device(
    tokens,
    lengths,
    states,
    norm_gain,
    mix_weight,
    rate_weight,
    decay_rate,
    head_gain,
    out_weight,
    final_gain,
    vocab_table,
    next_token,
):
    sequences = lengths.shape[0]
    local_width = tokens.shape[1]
    model_width = norm_gain.shape[0]
    blocks = lax.all_gather(tokens, HEAD, axis=0)
    normed, new_state = mixer(
        lengths,
        decay_rate,
        blocks,
        norm_gain.reshape(-1, N),
        mix_weight,
        rate_weight.T,
        head_gain.reshape(1, N),
        states[:, 0],
    )
    new_state = new_state[:, None]
    columns = lax.all_to_all(out_weight, HEAD, split_axis=1, concat_axis=0, tiled=True)
    mix_sum = jnp.dot(
        lax.all_gather(normed, HEAD, axis=1, tiled=True),
        columns,
        preferred_element_type=jnp.float32,
    )
    mixed = (tokens.astype(jnp.float32) + mix_sum).astype(jnp.bfloat16)
    last_index = (lengths - 1)[:, None, None]
    last_rows = jnp.take_along_axis(
        mixed.reshape(sequences, NEW_POSITIONS, local_width), last_index, axis=1
    )[:, 0]
    gathered = lax.all_gather(last_rows[None], BATCH_HEAD, axis=0, tiled=True)
    batch_count = lax.axis_size(BATCH)
    head_count = lax.axis_size(HEAD)
    everyone = gathered.reshape(batch_count, head_count, sequences, local_width).transpose(
        0, 2, 1, 3
    )
    everyone = everyone.reshape(batch_count * sequences, model_width)
    widened_all = everyone.astype(jnp.float32)
    factor = lax.rsqrt(jnp.mean(widened_all * widened_all, axis=1, keepdims=True) + ROW_EPSILON)
    hidden = (widened_all * factor * final_gain).astype(jnp.bfloat16)
    logits = jnp.dot(hidden, vocab_table.T, preferred_element_type=jnp.float32)
    vocab_here = vocab_table.shape[0]
    vocab_ids = lax.axis_index(BATCH_HEAD) * vocab_here + jnp.arange(vocab_here)
    largest = jnp.max(logits, axis=1)
    exp_total = jnp.sum(jnp.exp(logits - largest[:, None]), axis=1)
    target = jnp.sum(jnp.where(vocab_ids[None, :] == next_token[:, None], logits, 0.0), axis=1)
    largest, exp_total, target = joined_all(
        (largest, exp_total, target), BATCH_HEAD, combine_totals
    )
    return (mixed, new_state, target - (largest + jnp.log(exp_total)))


def solution(mesh):
    torus = Mesh(mesh.devices.reshape(8, 4, 8, 2), ("batch_0", "batch_1", "head_0", "head_1"))
    placed = (
        P(BATCH, HEAD),
        P(BATCH),
        P(BATCH, HEAD, None, None),
        P(),
        P(None, HEAD),
        P(None, HEAD),
        P(HEAD),
        P(),
        P(HEAD, None),
        P(),
        P(BATCH_HEAD, None),
        P(),
    )
    return jax.shard_map(
        on_device,
        mesh=torus,
        in_specs=placed,
        out_specs=(P(BATCH, HEAD), P(BATCH, HEAD, None, None), P()),
        check_vma=False,
    )
```

```python
import functools
import jax
import jax.numpy as jnp
from jax import lax
from jax.experimental import pallas as pl
from jax.experimental.pallas import tpu as pltpu
from jax.sharding import Mesh
from jax.sharding import PartitionSpec as P

BF = jnp.bfloat16
F32 = jnp.float32
HI = lax.Precision.HIGHEST
N = 128
CH = 32
NC = N // CH
LEVELS = 7
ROW_EPSILON = 1e-05
KEY_EPSILON = 1e-06


def split(x):
    high = x.astype(BF)
    return high, (x - high.astype(F32)).astype(BF)


def left_of(x):
    high, low = split(x)
    return jnp.concatenate([high, low], axis=1)


def right_of(x):
    high, low = split(x)
    both = jnp.concatenate([high, low], axis=1)
    return jnp.concatenate([both, both], axis=0)


def halves(product):
    return product[:, :N] + product[:, N:]


def dot(a, b):
    return jnp.dot(a, b, preferred_element_type=F32)


def dot_nt(a, b):
    return lax.dot_general(a, b, (((1,), (1,)), ((), ())), preferred_element_type=F32)


def fill_tables(masks, tri, picks):
    row = lax.broadcasted_iota(jnp.int32, (N, N), 0)
    col = lax.broadcasted_iota(jnp.int32, (N, N), 1)
    j, p, jj, pp = row // CH, row % CH, col // CH, col % CH
    steps = (j < 3) & (jj < 3)
    sets = [steps & (p == pp) & (j == 1) & (jj == 0), steps & (p == pp) & (j == 2) & (jj < 2)]
    for k in range(5):
        same = (p >> (k + 1)) == (pp >> (k + 1))
        sets.append(steps & same & (((p >> k) & 1) == 1) & (((pp >> k) & 1) == 0))
    sets.append((j == 3) & (jj < 3))
    for k, chosen in enumerate(sets):
        masks[k] = chosen.astype(F32)
    strict = steps & ((p > pp) | ((p == pp) & (j > jj)))
    masks[LEVELS + 1] = (strict | ((j == 3) & (jj < 3) & (p >= pp))).astype(F32)
    tri[...] = ((j == jj) & (pp <= p)).astype(F32)
    for c in range(NC):
        picks[:, c * N : (c + 1) * N] = ((j == c) & (p <= pp)).astype(F32)


def silu(v):
    return v / (1.0 + jnp.exp(-v))


def softplus(v):
    return jnp.maximum(v, 0.0) + jnp.log1p(jnp.exp(-jnp.abs(v)))


def place_rates(rate_t, weight, blank):
    width = weight.shape[1] - N
    blank[...] = jnp.zeros((N, N), F32)
    for b in range(rate_t.shape[1] // N):
        blank[0:4, :] = rate_t[:, b * N : (b + 1) * N].astype(F32)
        weight[b * N : (b + 1) * N, width:] = blank[...].T.astype(BF)


def widen(owners, fresh, blocks, gain, xs, squares):
    total = None
    for k, owner in enumerate(owners):
        for core in range(2):
            wide = blocks[owner * 2 + core].astype(F32)
            total = wide * wide if total is None else total + wide * wide
            at = (2 * k + core) * N
            xs[:, at : at + N] = (wide * gain[pl.ds(owner * 2 + core, 1), :]).astype(BF)
    squares[...] = total if fresh else squares[...] + total


def absorb(owners, fresh, half, weight, xs, acc):
    cols = slice(half * 4 * N, (half + 1) * 4 * N)
    kernel = jnp.concatenate(
        [weight[pl.ds(pl.multiple_of(o * 2 * N, 2 * N), 2 * N), cols] for o in owners], axis=0
    )
    product = dot(xs[:, : 2 * N * len(owners)], kernel)
    acc[:, cols] = product if fresh else acc[:, cols] + product


def sequence_inputs(s, length, rate, count, acc, squares, masks, tri, picks, la, tt, tmp, xh, xl, kt, eq, et):
    rows = slice(s * N, (s + 1) * N)
    total = jnp.sum(squares[rows, :], axis=1, keepdims=True)
    inverse = lax.rsqrt(total / (count * N) + ROW_EPSILON)
    projected = acc[rows, : 7 * N] * inverse
    rates = acc[rows, 7 * N :] * inverse
    query = silu(projected[:, :N])
    keys, values = [], []
    for j in range(3):
        key = silu(projected[:, (1 + j) * N : (2 + j) * N])
        keys.append(key * lax.rsqrt(jnp.sum(key * key, axis=1, keepdims=True) + KEY_EPSILON))
        values.append(silu(projected[:, (4 + j) * N : (5 + j) * N]))
    valid = lax.broadcasted_iota(jnp.int32, (N, 1), 0) < length
    betas = [
        jnp.broadcast_to(jnp.where(valid, 2.0 * jax.nn.sigmoid(rates[:, j : j + 1]), 0.0), (N, N))
        for j in range(3)
    ]
    decay = jnp.where(valid, -rate * softplus(rates[:, 3:4]), 0.0)
    decay = jnp.broadcast_to(decay, (N, N))
    cum = jnp.dot(tri[...], decay, precision=HI, preferred_element_type=F32)
    cum_row = jnp.dot(decay.T[:8], picks[...], precision=HI, preferred_element_type=F32)
    grow = jnp.exp(cum)
    one = jnp.ones((CH, N), F32)
    zero = jnp.zeros((CH, N), F32)
    eye = (
        lax.broadcasted_iota(jnp.int32, (N, N), 0) == lax.broadcasted_iota(jnp.int32, (N, N), 1)
    ).astype(F32)
    causal = masks[LEVELS + 1] > 0.5
    first = masks[0]
    for c in range(NC):
        at = slice(c * CH, (c + 1) * CH)
        n = s * NC + c
        kq = jnp.concatenate([keys[0][at], keys[1][at], keys[2][at], query[at]], axis=0)
        vv = jnp.concatenate([values[0][at], values[1][at], values[2][at], zero], axis=0)
        bb = jnp.concatenate([betas[0][at], betas[1][at], betas[2][at], one], axis=0)
        cc = jnp.concatenate([cum[at]] * 4, axis=0)
        gg = jnp.concatenate([grow[at]] * 3 + [zero], axis=0)
        high, low = split(kq)
        gram = halves(
            dot_nt(
                jnp.concatenate([high, low], axis=1),
                jnp.concatenate(
                    [jnp.concatenate([high, high], axis=1), jnp.concatenate([low, low], axis=1)],
                    axis=0,
                ),
            )
        )
        ratio = jnp.exp(jnp.where(causal, cc - cum_row[0:1, c * N : (c + 1) * N], -1e30))
        system = bb * ratio * gram
        la[n] = system
        pairs = system * first
        scale = jnp.sum(pairs[CH : 2 * CH], axis=0, keepdims=True)
        third = system[2 * CH : 3 * CH] * masks[1, 2 * CH : 3 * CH, :]
        third = third - pltpu.roll(third, N - CH, 1) * scale
        start = eye - pairs
        tt[n] = jnp.concatenate([start[: 2 * CH], start[2 * CH : 3 * CH] - third, start[3 * CH :]], axis=0)
        tmp[n] = jnp.zeros((N, N), F32)
        xa, xb = bb * vv, bb * gg * kq
        ha, lo_a = split(xa)
        hb, lo_b = split(xb)
        xh[n] = jnp.concatenate([ha, hb], axis=1)
        xl[n] = jnp.concatenate([lo_a, lo_b], axis=1)
        last = cum[(c + 1) * CH - 1 : (c + 1) * CH, :]
        tail = jnp.concatenate([jnp.exp(last - cum[at])] * 3 + [zero], axis=0)
        kt[n] = left_of((tail * kq).T)
        eq[n] = grow[at] * query[at]
        et[n] = jnp.broadcast_to(jnp.exp(last), (8, N))


def invert(ids, first, stop, masks, la, tt, tmp):
    top = 3 * CH

    def level(k, carry):
        mask = masks[k, :top, :]
        for n in ids:
            tmp[n, :top, :] = halves(dot(left_of(la[n, :top, :] * mask), right_of(tt[n])))
        for n in ids:
            t = tt[n, :top, :]
            tt[n, :top, :] = t - halves(dot(left_of(t), right_of(tmp[n])))
        return carry

    lax.fori_loop(first, stop, level, 0)
    if stop < LEVELS:
        return
    for n in ids:
        tt[n, top:, :] = -halves(dot(left_of(la[n, top:, :]), right_of(tt[n])))


def chunk_maps(n, tt, xh, xl, kt, eq, et, pq, rr, ov):
    high, low = split(tt[n])
    big = jnp.concatenate([high, low], axis=1)
    z = dot(big, jnp.concatenate([xh[n], xh[n]], axis=0)) + dot(high, xl[n])
    zh, zl = split(z)
    k = kt[n]
    maps = dot(k, jnp.concatenate([zh, zh], axis=0)) + dot(k[:, :N], zl)
    eye = (
        lax.broadcasted_iota(jnp.int32, (N, N), 0) == lax.broadcasted_iota(jnp.int32, (N, N), 1)
    ).astype(F32)
    p = eye * et[n, 0:1, :] - maps[:, N:]
    pq[n] = left_of(jnp.concatenate([p, eq[n] + z[3 * CH :, N:]], axis=0))
    rr[n] = maps[:, :N]
    ov[n] = -z[3 * CH :, :N]


def run_chain(sequences, states, new_state, normed, head_gain, pq, rr, ov):
    carried = [states[s].T for s in sequences]
    for c in range(NC):
        for k, s in enumerate(sequences):
            n = s * NC + c
            both = halves(dot(pq[n], right_of(carried[k])))
            carried[k] = both[:N] + rr[n]
            attended = both[N:] + ov[n]
            factor = lax.rsqrt(jnp.mean(attended * attended, axis=1, keepdims=True) + ROW_EPSILON)
            normed[s * N + c * CH : s * N + (c + 1) * CH, :] = (
                attended * factor * head_gain[...]
            ).astype(BF)
    for k, s in enumerate(sequences):
        new_state[s] = carried[k].T


def mixer_scratch(seqs, count, width):
    m = seqs * NC
    return [
        pltpu.VMEM((LEVELS + 2, N, N), F32),
        pltpu.VMEM((N, N), F32),
        pltpu.VMEM((N, NC * N), F32),
        pltpu.VMEM((seqs * N, 4 * N), BF),
        pltpu.VMEM((seqs * N, 8 * N), F32),
        pltpu.VMEM((seqs * N, N), F32),
        pltpu.VMEM((m, N, N), F32),
        pltpu.VMEM((m, N, N), F32),
        pltpu.VMEM((m, N, N), F32),
        pltpu.VMEM((m, N, 2 * N), BF),
        pltpu.VMEM((m, N, 2 * N), BF),
        pltpu.VMEM((m, N, 2 * N), BF),
        pltpu.VMEM((m, CH, N), F32),
        pltpu.VMEM((m, 8, N), F32),
        pltpu.VMEM((m, N + CH, 2 * N), BF),
        pltpu.VMEM((m, N, N), F32),
        pltpu.VMEM((m, CH, N), F32),
    ]


SEQS = 4
PARTS = 4
VOCAB_HERE = 32
SOURCES = 32
Z, X, Y, C = "batch_0", "batch_1", "head_0", "head_1"
HEAD = (Y, C)
BATCH = (Z, X)
BATCH_HEAD = (Z, X, Y, C)
MESH = pl.DeviceIdType.MESH


def remote(src, dst, send_sem, recv_sem, **place):
    return pltpu.make_async_remote_copy(
        src_ref=src,
        dst_ref=dst,
        send_sem=send_sem,
        recv_sem=recv_sem,
        device_id=place,
        device_id_type=MESH,
    )


def send(src, dst, send_sem, recv_sem, **place):
    copy = remote(src, dst, send_sem, recv_sem, **place)
    copy.start()
    return copy


def arrived(dst, recv_sem):
    pltpu.make_async_remote_copy(
        src_ref=dst,
        dst_ref=dst,
        send_sem=recv_sem,
        recv_sem=recv_sem,
        device_id={C: lax.axis_index(C)},
        device_id_type=MESH,
    ).wait_recv()


def wrap(index, size):
    return lax.rem(index + size, size)


class Ring:
    def __init__(self, buf, sems, ny):
        self.buf, self.ny = buf, ny
        self.s_right, self.r_right, self.s_left, self.r_left, self.s_pair, self.r_pair = sems
        self.y, self.c = lax.axis_index(Y), lax.axis_index(C)
        long, short = ny // 2, (ny - 1) // 2
        self.steps = [(long, short) if s % 2 == 0 else (short, long) for s in range(PARTS)]
        self.last = long - 1

    def piece(self, owner, core, s):
        size = self.buf.shape[1] // PARTS
        return self.buf.at[owner * 2 + core, pl.ds(s * size, size), :]

    def owner(self, way, k):
        return wrap(self.y - (k + 1), self.ny) if way == 0 else wrap(self.y + (k + 1), self.ny)

    def pair_index(self, way, k, s):
        return (1 + k if way == 0 else 1 + self.steps[s][0] + k) * PARTS + s

    def hop(self, way, k, s):
        piece = self.piece(self.owner(way, k - 1), self.c, s)
        to = wrap(self.y + 1, self.ny) if way == 0 else wrap(self.y - 1, self.ny)
        ss, rs = (self.s_right, self.r_right) if way == 0 else (self.s_left, self.r_left)
        at = k * PARTS + s
        return remote(piece, piece, ss.at[at], rs.at[at], **{Y: to})

    def to_pair(self, way, k, s):
        piece = self.piece(self.owner(way, k), self.c, s)
        at = self.pair_index(way, k, s)
        return remote(piece, piece, self.s_pair.at[at], self.r_pair.at[at], **{C: 1 - self.c})

    def start(self):
        for s in range(PARTS):
            for way in range(2):
                if self.steps[s][way] > 0:
                    self.hop(way, 0, s).start()
        for s in range(PARTS):
            self.to_pair(0, -1, s).start()

    def forward(self, k, s):
        for way in range(2):
            if k < self.steps[s][way]:
                owner = self.owner(way, k)
                at = k * PARTS + s
                arrived(self.piece(owner, self.c, s), (self.r_right, self.r_left)[way].at[at])
                if k + 1 < self.steps[s][way]:
                    self.hop(way, k + 1, s).start()
                self.to_pair(way, k, s).start()

    def step(self, k):
        for s in range(PARTS):
            self.forward(k, s)

    def wait_pair(self, way, k):
        for s in range(PARTS):
            at = way if k < self.steps[s][way] else 1 - way
            piece = self.piece(self.owner(at, k), 1 - self.c, s)
            arrived(piece, self.r_pair.at[self.pair_index(at, k, s)])

    def owners(self, k):
        return [(0, k), (1, k)] if 2 * (k + 1) < self.ny else [(0, k)]

    def wait_all_pairs(self):
        self.wait_pair(0, -1)
        for k in range(self.last + 1):
            for way, step in self.owners(k):
                self.wait_pair(way, step)

    def drain(self):
        for s in range(PARTS):
            self.to_pair(0, -1, s).wait_send()
            for way in range(2):
                for k in range(self.steps[s][way]):
                    self.hop(way, k, s).wait_send()
                    self.to_pair(way, k, s).wait_send()


def exchange_head(buf, mine, sems, ny):
    y, c = lax.axis_index(Y), lax.axis_index(C)
    sent = []
    order = sorted(range(1, 2 * ny), key=lambda k: -min(k // 2, ny - k // 2))
    for k in order:
        to = {Y: wrap(y + k // 2, ny), C: lax.rem(c + k % 2, 2)}
        sent.append(send(buf.at[mine], buf.at[mine], sems[0].at[k - 1], sems[1].at[k - 1], **to))
    return sent


def await_head(buf, sems, ny):
    y, c = lax.axis_index(Y), lax.axis_index(C)
    for k in range(1, 2 * ny):
        source = wrap(y - k // 2, ny) * 2 + lax.rem(c + k % 2, 2)
        arrived(buf.at[source], sems[1].at[k - 1])


def exchange_axis(axis, size, piece, sems):
    me = lax.axis_index(axis)
    order = sorted(range(1, size), key=lambda k: -min(k, size - k))
    return [
        send(piece(me), piece(me), sems[0].at[k - 1], sems[1].at[k - 1], **{axis: wrap(me + k, size)})
        for k in order
    ]


def await_axis(axis, size, piece, sems):
    me = lax.axis_index(axis)
    for k in range(1, size):
        arrived(piece(wrap(me - k, size)), sems[1].at[k - 1])


def combine(buf, count):
    parts = [buf[k] for k in range(count)]
    top = functools.reduce(jnp.maximum, [part[0:1] for part in parts])
    total = sum(part[1:2] * jnp.exp(part[0:1] - top) for part in parts)
    target = sum(part[2:3] for part in parts)
    return top, total, target


def put_stats(buf, at, top, total, target):
    buf[at] = jnp.concatenate([top, total, target, jnp.zeros_like(top)], axis=0)


NAMES = (
    "masks", "tri", "picks", "xs", "acc", "squares", "la", "tt", "tmp", "xh", "xl", "kt", "eq", "et", "pq",
    "rr", "ov", "blocks", "nall", "weight", "cols", "vocab", "state", "blank", "lastn",
    "lastm", "shaped", "hid", "part", "other", "sy", "sp", "tr1", "tr2", "tr3", "tr4",
    "tr5", "tr6", "nr1", "nr2", "nr3", "nr4", "nr5", "nr6", "c1", "c2", "d1", "d2", "v1", "v2", "a1",
    "a2", "b1", "b2", "z1", "z2", "x1", "x2", "p1", "p2", "g1", "g2", "h1", "h2",
    "local", "free", "gain", "rates", "hgain", "fgain", "wanted", "length", "rate",
)


def one_kernel(sizes, *refs):
    (tokens, lengths_in, states, gain_in, mix_weight, rate_in, decay_in, head_in, out_weight,
     final_in, vocab_table, next_in, mixed, new_state, likelihood) = refs[:15]
    r = dict(zip(NAMES, refs[15:]))
    nz, nx, ny = sizes
    heads = 2 * ny
    z, x, y, c = (lax.axis_index(a) for a in BATCH_HEAD)
    me = y * 2 + c
    blocks, nall, cols, hid = r["blocks"], r["nall"], r["cols"], r["hid"]
    local = r["local"]
    gain, rate_t, head_gain, final_gain = r["gain"], r["rates"], r["hgain"], r["fgain"]
    next_token, lengths, rate = r["wanted"], r["length"], r["rate"]
    weight, acc, squares_of = r["weight"], r["acc"], r["squares"]

    own = pltpu.make_async_copy(tokens, blocks.at[me], local.at[0])
    own.start()
    small = []
    for k, (src, dst) in enumerate((
        (gain_in, gain), (rate_in, rate_t), (head_in, head_gain), (final_in, final_gain),
        (next_in, next_token), (lengths_in, lengths), (decay_in, rate),
    )):
        small.append(pltpu.make_async_copy(src, dst, local.at[8 + k]))
        small[-1].start()
    load_weight = pltpu.make_async_copy(mix_weight, weight.at[:, pl.ds(0, 7 * N)], local.at[1])
    load_weight.start()
    load_state = pltpu.make_async_copy(states, r["state"], local.at[2])
    load_state.start()
    band = N // nx
    rows_here = pl.ds(pl.multiple_of(x * band, band), band)
    own_cols = pltpu.make_async_copy(
        out_weight.at[rows_here, pl.ds(pl.multiple_of(me * N, N), N)],
        cols.at[me, rows_here, :],
        local.at[3],
    )
    own_cols.start()
    quarter = heads * N // 8
    vocab_copies = []

    def vocab_piece(half, q):
        start = pl.multiple_of(half * (4 * quarter) + q * quarter, N)
        rows = pl.ds(pl.multiple_of(q * 2 * VOCAB_HERE + c * VOCAB_HERE, VOCAB_HERE), VOCAB_HERE)
        return vocab_table.at[:, pl.ds(start, quarter)], r["vocab"].at[rows, :]

    for q in range(4):
        src, dst = vocab_piece(c, q)
        copy = pltpu.make_async_copy(src, dst, local.at[4 + q])
        copy.start()
        vocab_copies.append(copy)
    if nz * nx < SOURCES:
        hid[...] = jnp.zeros_like(hid)

    barrier = pltpu.get_barrier_semaphore()
    near = [{C: 1 - c}]
    for axis, size, at in ((Y, ny, y), (Z, nz, z), (X, nx, x)):
        if size > 1:
            near += [{axis: wrap(at + 1, size)}, {axis: wrap(at - 1, size)}]
    for place in near:
        pl.semaphore_signal(barrier, inc=1, device_id=place, device_id_type=MESH)
    own.wait()
    pl.semaphore_wait(barrier, len(near))

    ring = Ring(blocks, [r[f"tr{k}"] for k in range(1, 7)], ny)
    ring.start()
    pair_vocab = []
    for q in range(4):
        src, dst = vocab_piece(1 - c, q)
        pair_vocab.append(send(src, dst, r["v1"].at[q], r["v2"].at[q], **{C: 1 - c}))

    pending = []
    free = r["free"]
    for slot, (axis, size, at) in enumerate(((X, nx, x), (Z, nz, z))):
        for _ in range(size - 1):
            def signal(slot=slot, axis=axis, size=size, at=at):
                pl.semaphore_signal(
                    free.at[slot], inc=1, device_id={axis: wrap(at + 1, size)}, device_id_type=MESH
                )

            def await_signal(slot=slot):
                pl.semaphore_wait(free.at[slot], 1)

            pending += [signal, await_signal]

    def plane_step():
        if pending:
            pending.pop(0)()

    def plane_next():
        plane_step()
        plane_step()

    if pending:
        plane_step()
    fill_tables(r["masks"], r["tri"], r["picks"])
    for copy in small:
        copy.wait()
    place_rates(rate_t, weight, r["blank"])
    load_weight.wait()

    def ready(arrivals):
        for way, k in arrivals:
            ring.wait_pair(way, k)
        owners = [ring.owner(way, k) for way, k in arrivals]
        fresh = arrivals[0][1] < 0
        widen(owners, fresh, blocks, gain, r["xs"], squares_of)
        return owners, fresh

    def take(owners, fresh, half):
        absorb(owners, fresh, half, weight, r["xs"], acc)

    for k in range(ring.last + 1):
        half = PARTS // 2
        for s in range(half):
            ring.forward(k, s)
        found = ready([(0, -1)] if k == 0 else ring.owners(k - 1))
        take(*found, 0)
        for s in range(half, PARTS):
            ring.forward(k, s)
        take(*found, 1)
        plane_next()

    col_sent = []
    for k in range(1, heads):
        py, pc = wrap(y + k // 2, ny), lax.rem(c + k % 2, 2)
        to = pl.multiple_of((py * 2 + pc) * N, N)
        col_sent.append(
            send(out_weight.at[rows_here, pl.ds(to, N)], cols.at[me, rows_here, :],
                 r["c1"].at[k - 1], r["c2"].at[k - 1], **{Y: py, C: pc})
        )
    found = ready(ring.owners(ring.last))
    take(*found, 0)
    take(*found, 1)
    for s in range(SEQS):
        plane_next()
        sequence_inputs(
            s, lengths[s], rate[0], heads, acc, squares_of, r["masks"], r["tri"], r["picks"],
            r["la"], r["tt"], r["tmp"], r["xh"], r["xl"], r["kt"], r["eq"], r["et"],
        )
    plane_next()
    ids = range(SEQS * NC)
    invert(ids, 2, 5, r["masks"], r["la"], r["tt"], r["tmp"])
    plane_next()
    own_cols.wait()
    for k in range(1, heads):
        source = wrap(y - k // 2, ny) * 2 + lax.rem(c + k % 2, 2)
        arrived(cols.at[source, rows_here, :], r["c2"].at[k - 1])
    bands = cols.at[:, rows_here, :]
    for dx in range(1, nx):
        col_sent.append(
            send(bands, bands, r["d1"].at[dx - 1], r["d2"].at[dx - 1], **{X: wrap(x + dx, nx)})
        )
    invert(ids, 5, LEVELS, r["masks"], r["la"], r["tt"], r["tmp"])
    plane_next()
    for n in ids:
        chunk_maps(
            n, r["tt"], r["xh"], r["xl"], r["kt"], r["eq"], r["et"], r["pq"], r["rr"], r["ov"]
        )
    load_state.wait()
    plane_next()
    run_chain(
        range(SEQS), r["state"], new_state, nall.at[me], head_gain, r["pq"], r["rr"], r["ov"]
    )

    position = lax.broadcasted_iota(jnp.int32, (N, N), 0)

    def last_rows(ref):
        rows = []
        for s in range(SEQS):
            wide = ref[me, s * N : (s + 1) * N, :].astype(F32)
            kept = jnp.where(position == lengths[s] - 1, wide, 0.0)
            rows.append(jnp.sum(kept, axis=0, keepdims=True))
        return jnp.concatenate(rows, axis=0)

    lastn, lastm = r["lastn"], r["lastm"]
    lastn[me] = last_rows(nall)
    sends = exchange_head(lastn, me, (r["a1"], r["a2"]), ny)
    bulk = Ring(nall, [r[f"nr{k}"] for k in range(1, 7)], ny)
    residual = last_rows(blocks)
    for dx in range(1, nx):
        theirs = pl.ds(pl.multiple_of(wrap(x - dx, nx) * band, band), band)
        arrived(cols.at[:, theirs, :], r["d2"].at[dx - 1])
    await_head(lastn, (r["a1"], r["a2"]), ny)
    wide = jnp.concatenate([lastn[b].astype(BF) for b in range(heads)], axis=1)
    every_col = jnp.concatenate([cols[b] for b in range(heads)], axis=0)
    lastm[me] = (residual + dot(wide, every_col)).astype(BF).astype(F32)
    sends += exchange_head(lastm, me, (r["b1"], r["b2"]), ny)
    bulk.start()
    late = list(range(ring.last + 1))

    def bulk_step():
        if late:
            bulk.step(late.pop(0))

    while pending:
        plane_step()
    await_head(lastm, (r["b1"], r["b2"]), ny)
    squares = sum(lastm[b] * lastm[b] for b in range(heads))
    factor = lax.rsqrt(jnp.sum(squares, axis=1, keepdims=True) / (heads * N) + ROW_EPSILON)
    per = heads // 8
    shaped = r["shaped"]
    for q in range(4):
        for k in range(per):
            b = c * (heads // 2) + q * per + k
            shaped[q * SEQS : (q + 1) * SEQS, k * N : (k + 1) * N] = (
                lastm[b] * factor * final_gain[pl.ds(b, 1), :]
            )
    slot = x * nz + z
    hid[slot] = shaped[...].astype(BF)
    def cell(px, pz):
        return hid.at[px * nz + pz]

    def to_row(pz, k):
        for dx in range(1, nx):
            at = (dx - 1) * nz + k
            sends.append(
                send(cell(x, pz), cell(x, pz), r["x1"].at[at], r["x2"].at[at], **{X: wrap(x + dx, nx)})
            )

    sends += exchange_axis(Z, nz, lambda pz: cell(x, pz), (r["z1"], r["z2"]))
    to_row(z, 0)
    bulk_step()
    for k in sorted(range(1, nz), key=lambda k: min(k, nz - k)):
        pz = wrap(z - k, nz)
        arrived(cell(x, pz), r["z2"].at[k - 1])
        to_row(pz, k)
    bulk_step()
    for q in range(4):
        vocab_copies[q].wait()
        rows = pl.ds(
            pl.multiple_of(q * 2 * VOCAB_HERE + (1 - c) * VOCAB_HERE, VOCAB_HERE), VOCAB_HERE
        )
        arrived(r["vocab"].at[rows, :], r["v2"].at[q])
    lane = lax.broadcasted_iota(jnp.int32, (N, N), 1)
    rank = lax.broadcasted_iota(jnp.int32, (N, N), 0)
    source = ((lane // 4) % 4) * 8 + lane // 16
    order = (lax.rem(source, nz) * nx + source // nz) * SEQS + lane % 4
    permute = ((order == rank) & (source < nz * nx)).astype(F32)
    wanted = jnp.broadcast_to(next_token[...].astype(F32), (8, N))
    wanted = jnp.dot(wanted, permute, precision=HI, preferred_element_type=F32)[0:1]
    wanted = (wanted + 0.5).astype(jnp.int32)
    for dx in range(1, nx):
        for k in range(nz):
            arrived(cell(wrap(x - dx, nx), wrap(z - k, nz)), r["x2"].at[(dx - 1) * nz + k])

    everyone = jnp.concatenate([hid[k] for k in range(SOURCES)], axis=0)
    product = dot_nt(r["vocab"][...], everyone)
    height = 2 * VOCAB_HERE
    quarter_of = (lane[:height] % 16) // 4
    packed = jnp.zeros((height, N), F32)
    for k in range(4):
        mine = jnp.zeros((height, N), F32)
        for q in range(4):
            block = product[q * height : (q + 1) * height, k * N : (k + 1) * N]
            mine = mine + jnp.where(quarter_of == q, block, 0.0)
        mine = mine + pltpu.roll(mine, N - 4, 1)
        mine = mine + pltpu.roll(mine, N - 8, 1)
        if k:
            mine = pltpu.roll(mine, 4 * k, 1)
        packed = packed + jnp.where(quarter_of == k, mine, 0.0)
    part, other = r["part"], r["other"]
    part[0] = packed[:VOCAB_HERE]
    part[1] = packed[VOCAB_HERE:]
    sends.append(send(part.at[1 - c], other, r["p1"].at[0], r["p2"].at[0], **{C: 1 - c}))
    arrived(other, r["p2"].at[0])
    logits = part[c] + other[...]
    vocab_ids = (((z * nx + x) * ny + y) * 2 + c) * VOCAB_HERE + rank[:VOCAB_HERE]
    top = jnp.max(logits, axis=0, keepdims=True)
    total = jnp.sum(jnp.exp(logits - top), axis=0, keepdims=True)
    target = jnp.sum(jnp.where(vocab_ids == wanted, logits, 0.0), axis=0, keepdims=True)
    sy, sp = r["sy"], r["sp"]
    put_stats(sy, me, top, total, target)
    sends += exchange_head(sy, me, (r["g1"], r["g2"]), ny)
    bulk_step()
    await_head(sy, (r["g1"], r["g2"]), ny)
    put_stats(sp, slot, *combine(sy, heads))
    far = sorted(
        (k for k in range(1, nz * nx)),
        key=lambda k: -min(k % nz, nz - k % nz) - min(k // nz, nx - k // nz),
    )
    for k in far:
        to = {Z: wrap(z + k % nz, nz), X: wrap(x + k // nz, nx)}
        sends.append(send(sp.at[slot], sp.at[slot], r["h1"].at[k - 1], r["h2"].at[k - 1], **to))
    while late:
        bulk_step()
    bulk.wait_all_pairs()

    def mix(s, carry):
        rows = pl.ds(pl.multiple_of(s * N, N), N)
        wide = jnp.concatenate([nall[b, rows, :] for b in range(heads)], axis=1)
        every = jnp.concatenate([cols[b] for b in range(heads)], axis=0)
        mixed[rows, :] = (blocks[me, rows, :].astype(F32) + dot(wide, every)).astype(BF)
        return carry

    lax.fori_loop(0, SEQS, mix, 0)
    ring.drain()
    bulk.drain()
    for copy in col_sent + pair_vocab:
        copy.wait_send()
    for k in range(1, nz * nx):
        arrived(sp.at[wrap(x - k // nz, nx) * nz + wrap(z - k % nz, nz)], r["h2"].at[k - 1])
    top, total, target = combine(sp, nz * nx)
    result = jnp.broadcast_to(target - (top + jnp.log(total)), (8, N))
    likelihood[...] = lax.dot_general(
        result, permute, (((1,), (1,)), ((), ())), precision=HI, preferred_element_type=F32
    )[0:1]
    for copy in sends:
        copy.wait_send()


def deliver_kernel(*refs):
    sems = refs[-1]
    copies = [pltpu.make_async_copy(refs[k], refs[3 + k], sems.at[k]) for k in range(3)]
    for copy in copies:
        copy.start()
    for copy in copies:
        copy.wait()


def deliver(*arrays):
    return pl.pallas_call(
        deliver_kernel,
        out_shape=tuple(jax.ShapeDtypeStruct(a.shape, a.dtype) for a in arrays),
        in_specs=[pl.BlockSpec(memory_space=pltpu.VMEM)] * 3,
        out_specs=(pl.BlockSpec(memory_space=pl.ANY),) * 3,
        scratch_shapes=[pltpu.SemaphoreType.DMA((3,))],
    )(*arrays)


def on_device(sizes, tokens, lengths, states, norm_gain, mix_weight, rate_weight, decay_rate,
              head_gain, out_weight, final_gain, vocab_table, next_token):
    nz, nx, ny = sizes
    heads = 2 * ny
    rows = SEQS * N
    everyone = next_token.shape[0]
    vmem = pl.BlockSpec(memory_space=pltpu.VMEM)
    hbm = pl.BlockSpec(memory_space=pltpu.HBM)
    dma = lambda n: pltpu.SemaphoreType.DMA((max(n, 1),))
    group = 2 * ny - 1
    scratch = mixer_scratch(SEQS, heads, mix_weight.shape[1]) + [
        pltpu.VMEM((heads, rows, N), BF),
        pltpu.VMEM((heads, rows, N), BF),
        pltpu.VMEM((heads * N, 8 * N), BF),
        pltpu.VMEM((heads, N, N), BF),
        pltpu.VMEM((8 * VOCAB_HERE, heads * N // 8), BF),
        pltpu.VMEM((SEQS, N, N), F32),
        pltpu.VMEM((N, N), F32),
        pltpu.VMEM((heads, SEQS, N), F32),
        pltpu.VMEM((heads, SEQS, N), F32),
        pltpu.VMEM((4 * SEQS, heads * N // 8), F32),
        pltpu.VMEM((SOURCES, 4 * SEQS, heads * N // 8), BF),
        pltpu.VMEM((2, VOCAB_HERE, N), F32),
        pltpu.VMEM((VOCAB_HERE, N), F32),
        pltpu.VMEM((heads, 4, N), F32),
        pltpu.VMEM((nz * nx, 4, N), F32),
    ]
    hops = PARTS * max(ny // 2, 1)
    scratch += [dma(hops)] * 4 + [dma(PARTS * ny)] * 2
    scratch += [dma(hops)] * 4 + [dma(PARTS * ny)] * 2
    scratch += [dma(group)] * 2 + [dma(nx - 1)] * 2 + [dma(4)] * 2 + [dma(group)] * 4
    scratch += [dma(nz - 1)] * 2 + [dma((nx - 1) * nz)] * 2 + [dma(1)] * 2
    scratch += [dma(group)] * 2 + [dma(nz * nx - 1)] * 2
    scratch += [dma(15), pltpu.SemaphoreType.REGULAR((2,))]
    scratch += [
        pltpu.VMEM((heads, N), F32),
        pltpu.VMEM((4, heads * N), BF),
        pltpu.VMEM((1, N), F32),
        pltpu.VMEM((heads, N), F32),
        pltpu.VMEM((1, N), jnp.int32),
        pltpu.SMEM((SEQS,), jnp.int32),
        pltpu.SMEM((1,), F32),
    ]
    wanted = next_token.reshape(1, everyone)
    if everyone < N:
        wanted = jnp.pad(wanted, ((0, 0), (0, N - everyone)))
    mixed, new_state, likelihood = pl.pallas_call(
        functools.partial(one_kernel, sizes),
        out_shape=(
            jax.ShapeDtypeStruct((rows, N), BF),
            jax.ShapeDtypeStruct((SEQS, N, N), F32),
            jax.ShapeDtypeStruct((1, N), F32),
        ),
        in_specs=[hbm] * 12,
        out_specs=(vmem, vmem, vmem),
        scratch_shapes=scratch,
        compiler_params=pltpu.CompilerParams(
            collective_id=0, has_side_effects=True, vmem_limit_bytes=63 * 1024 * 1024
        ),
    )(
        tokens,
        lengths,
        states[:, 0],
        norm_gain.reshape(heads, N),
        mix_weight,
        rate_weight.T,
        decay_rate,
        head_gain.reshape(1, N),
        out_weight,
        final_gain.reshape(heads, N),
        vocab_table,
        wanted,
    )
    mixed, new_state, likelihood = deliver(mixed, new_state, likelihood)
    return mixed, new_state[:, None], likelihood[0, :everyone]


def build(torus):
    sizes = (torus.shape[Z], torus.shape[X], torus.shape[Y])
    placed = (
        P(BATCH, HEAD),
        P(BATCH),
        P(BATCH, HEAD, None, None),
        P(),
        P(None, HEAD),
        P(None, HEAD),
        P(HEAD),
        P(),
        P(HEAD, None),
        P(),
        P(BATCH_HEAD, None),
        P(),
    )
    return jax.shard_map(
        functools.partial(on_device, sizes),
        mesh=torus,
        in_specs=placed,
        out_specs=(P(BATCH, HEAD), P(BATCH, HEAD, None, None), P()),
        check_vma=False,
    )


def solution(mesh):
    torus = Mesh(mesh.devices.reshape(8, 4, 8, 2), BATCH_HEAD)
    return build(torus)
```

```python
import functools
import jax
import jax.numpy as jnp
from jax import lax
from jax.experimental import pallas as pl
from jax.experimental.pallas import tpu as pltpu
from jax.sharding import Mesh
from jax.sharding import PartitionSpec as P

BF = jnp.bfloat16
F32 = jnp.float32
HI = lax.Precision.HIGHEST
N = 128
CH = 32
NC = N // CH
LEVELS = 7
ROW_EPSILON = 1e-05
KEY_EPSILON = 1e-06


def split(x):
    high = x.astype(BF)
    return high, (x - high.astype(F32)).astype(BF)


def left_of(x):
    high, low = split(x)
    return jnp.concatenate([high, low], axis=1)


def twice(both):
    return jnp.concatenate([both, both], axis=0)


def right_of(x):
    return twice(left_of(x))


def joined(both):
    return both[:, :N].astype(F32) + both[:, N:].astype(F32)


def halves(product):
    return product[:, :N] + product[:, N:]


def dot(a, b):
    return jnp.dot(a, b, preferred_element_type=F32)


def dot_nt(a, b):
    return lax.dot_general(a, b, (((1,), (1,)), ((), ())), preferred_element_type=F32)


def fill_tables(masks, levels, tri, picks):
    row = lax.broadcasted_iota(jnp.int32, (N, N), 0)
    col = lax.broadcasted_iota(jnp.int32, (N, N), 1)
    j, p, jj, pp = row // CH, row % CH, col // CH, col % CH
    steps = (j < 3) & (jj < 3)
    sets = [steps & (p == pp) & (j == 1) & (jj == 0), steps & (p == pp) & (j == 2) & (jj < 2)]
    for k in range(5):
        same = (p >> (k + 1)) == (pp >> (k + 1))
        sets.append(steps & same & (((p >> k) & 1) == 1) & (((pp >> k) & 1) == 0))
    sets.append((j == 3) & (jj < 3))
    for k, chosen in enumerate(sets):
        masks[k] = chosen.astype(F32)
        levels[k] = jnp.concatenate([chosen.astype(F32).astype(BF)] * 2, axis=1)
    strict = steps & ((p > pp) | ((p == pp) & (j > jj)))
    masks[LEVELS + 1] = (strict | ((j == 3) & (jj < 3) & (p >= pp))).astype(F32)
    tri[...] = ((j == jj) & (pp <= p)).astype(F32)
    for c in range(NC):
        picks[:, c * N : (c + 1) * N] = ((j == c) & (p <= pp)).astype(F32)


def silu(v):
    return v / (1.0 + jnp.exp(-v))


def softplus(v):
    return jnp.maximum(v, 0.0) + jnp.log1p(jnp.exp(-jnp.abs(v)))


def place_rates(rate_t, weight, blank):
    width = weight.shape[1] - N
    blank[...] = jnp.zeros((N, N), F32)
    for b in range(rate_t.shape[1] // N):
        blank[0:4, :] = rate_t[:, b * N : (b + 1) * N].astype(F32)
        weight[b * N : (b + 1) * N, width:] = blank[...].T.astype(BF)


def widen(owners, fresh, blocks, gain, xs, squares):
    total = None
    for k, owner in enumerate(owners):
        for core in range(2):
            wide = blocks[owner * 2 + core].astype(F32)
            total = wide * wide if total is None else total + wide * wide
            at = (2 * k + core) * N
            xs[:, at : at + N] = (wide * gain[pl.ds(owner * 2 + core, 1), :]).astype(BF)
    squares[...] = total if fresh else squares[...] + total


def absorb(owners, fresh, quarter, weight, xs, acc):
    cols = slice(quarter * 2 * N, (quarter + 1) * 2 * N)
    kernel = jnp.concatenate(
        [weight[pl.ds(pl.multiple_of(o * 2 * N, 2 * N), 2 * N), cols] for o in owners], axis=0
    )
    product = dot(xs[:, : 2 * N * len(owners)], kernel)
    acc[:, cols] = product if fresh else acc[:, cols] + product


def sequence_inputs(s, length, rate, count, acc, squares, masks, tri, picks, la, tt, tmp, xh, xl, kt, eq, et):
    rows = slice(s * N, (s + 1) * N)
    total = jnp.sum(squares[rows, :], axis=1, keepdims=True)
    inverse = lax.rsqrt(total / (count * N) + ROW_EPSILON)
    projected = acc[rows, : 7 * N] * inverse
    rates = acc[rows, 7 * N :] * inverse
    query = silu(projected[:, :N])
    keys, values = [], []
    for j in range(3):
        key = silu(projected[:, (1 + j) * N : (2 + j) * N])
        keys.append(key * lax.rsqrt(jnp.sum(key * key, axis=1, keepdims=True) + KEY_EPSILON))
        values.append(silu(projected[:, (4 + j) * N : (5 + j) * N]))
    valid = lax.broadcasted_iota(jnp.int32, (N, 1), 0) < length
    betas = [
        jnp.broadcast_to(jnp.where(valid, 2.0 * jax.nn.sigmoid(rates[:, j : j + 1]), 0.0), (N, N))
        for j in range(3)
    ]
    decay = jnp.where(valid, -rate * softplus(rates[:, 3:4]), 0.0)
    decay = jnp.broadcast_to(decay, (N, N))
    cum = jnp.dot(tri[...], decay, precision=HI, preferred_element_type=F32)
    cum_row = jnp.dot(decay.T[:8], picks[...], precision=HI, preferred_element_type=F32)
    grow = jnp.exp(cum)
    one = jnp.ones((CH, N), F32)
    zero = jnp.zeros((CH, N), F32)
    eye = (
        lax.broadcasted_iota(jnp.int32, (N, N), 0) == lax.broadcasted_iota(jnp.int32, (N, N), 1)
    ).astype(F32)
    causal = masks[LEVELS + 1] > 0.5
    first = masks[0]
    for c in range(NC):
        at = slice(c * CH, (c + 1) * CH)
        n = s * NC + c
        kq = jnp.concatenate([keys[0][at], keys[1][at], keys[2][at], query[at]], axis=0)
        vv = jnp.concatenate([values[0][at], values[1][at], values[2][at], zero], axis=0)
        bb = jnp.concatenate([betas[0][at], betas[1][at], betas[2][at], one], axis=0)
        cc = jnp.concatenate([cum[at]] * 4, axis=0)
        gg = jnp.concatenate([grow[at]] * 3 + [zero], axis=0)
        high, low = split(kq)
        gram = halves(
            dot_nt(
                jnp.concatenate([high, low], axis=1),
                jnp.concatenate(
                    [jnp.concatenate([high, high], axis=1), jnp.concatenate([low, low], axis=1)],
                    axis=0,
                ),
            )
        )
        ratio = jnp.exp(jnp.where(causal, cc - cum_row[0:1, c * N : (c + 1) * N], -1e30))
        system = bb * ratio * gram
        la[n] = left_of(system)
        pairs = system * first
        scale = jnp.sum(pairs[CH : 2 * CH], axis=0, keepdims=True)
        third = system[2 * CH : 3 * CH] * masks[1, 2 * CH : 3 * CH, :]
        third = third - pltpu.roll(third, N - CH, 1) * scale
        start = eye - pairs
        tt[n] = left_of(
            jnp.concatenate(
                [start[: 2 * CH], start[2 * CH : 3 * CH] - third, start[3 * CH :]], axis=0
            )
        )
        tmp[n] = jnp.zeros((N, 2 * N), BF)
        xa, xb = bb * vv, bb * gg * kq
        ha, lo_a = split(xa)
        hb, lo_b = split(xb)
        xh[n] = jnp.concatenate([ha, hb], axis=1)
        xl[n] = jnp.concatenate([lo_a, lo_b], axis=1)
        last = cum[(c + 1) * CH - 1 : (c + 1) * CH, :]
        tail = jnp.concatenate([jnp.exp(last - cum[at])] * 3 + [zero], axis=0)
        kt[n] = left_of((tail * kq).T)
        eq[n] = grow[at] * query[at]
        et[n] = jnp.broadcast_to(jnp.exp(last), (8, N))


def invert(ids, first, stop, levels, la, tt, tmp):
    top = 3 * CH

    def level(k, carry):
        mask = levels[k, :top, :]
        for n in ids:
            tmp[n, :top, :] = left_of(halves(dot(la[n, :top, :] * mask, twice(tt[n]))))
        for n in ids:
            t = tt[n, :top, :]
            tt[n, :top, :] = left_of(joined(t) - halves(dot(t, twice(tmp[n]))))
        return carry

    lax.fori_loop(first, stop, level, 0)
    if stop < LEVELS:
        return
    for n in ids:
        tt[n, top:, :] = left_of(-halves(dot(la[n, top:, :], twice(tt[n]))))


def chunk_maps(n, tt, xh, xl, kt, eq, et, pq, rr, ov):
    big = tt[n]
    high = big[:, :N]
    z = dot(big, jnp.concatenate([xh[n], xh[n]], axis=0)) + dot(high, xl[n])
    zh, zl = split(z)
    k = kt[n]
    maps = dot(k, jnp.concatenate([zh, zh], axis=0)) + dot(k[:, :N], zl)
    eye = (
        lax.broadcasted_iota(jnp.int32, (N, N), 0) == lax.broadcasted_iota(jnp.int32, (N, N), 1)
    ).astype(F32)
    p = eye * et[n, 0:1, :] - maps[:, N:]
    pq[n] = left_of(jnp.concatenate([p, eq[n] + z[3 * CH :, N:]], axis=0))
    rr[n] = maps[:, :N]
    ov[n] = -z[3 * CH :, :N]


def run_chain(sequences, states, new_state, normed, head_gain, pq, rr, ov):
    carried = [states[s].T for s in sequences]
    for c in range(NC):
        for k, s in enumerate(sequences):
            n = s * NC + c
            both = halves(dot(pq[n], right_of(carried[k])))
            carried[k] = both[:N] + rr[n]
            attended = both[N:] + ov[n]
            factor = lax.rsqrt(jnp.mean(attended * attended, axis=1, keepdims=True) + ROW_EPSILON)
            normed[s * N + c * CH : s * N + (c + 1) * CH, :] = (
                attended * factor * head_gain[...]
            ).astype(BF)
    for k, s in enumerate(sequences):
        new_state[s] = carried[k].T


def mixer_scratch(seqs, count, width):
    m = seqs * NC
    return [
        pltpu.VMEM((LEVELS + 2, N, N), F32),
        pltpu.VMEM((LEVELS + 1, N, 2 * N), BF),
        pltpu.VMEM((N, N), F32),
        pltpu.VMEM((N, NC * N), F32),
        pltpu.VMEM((seqs * N, 4 * N), BF),
        pltpu.VMEM((seqs * N, 8 * N), F32),
        pltpu.VMEM((seqs * N, N), F32),
        pltpu.VMEM((m, N, 2 * N), BF),
        pltpu.VMEM((m, N, 2 * N), BF),
        pltpu.VMEM((m, N, 2 * N), BF),
        pltpu.VMEM((m, N, 2 * N), BF),
        pltpu.VMEM((m, N, 2 * N), BF),
        pltpu.VMEM((m, N, 2 * N), BF),
        pltpu.VMEM((m, CH, N), F32),
        pltpu.VMEM((m, 8, N), F32),
        pltpu.VMEM((m, N + CH, 2 * N), BF),
        pltpu.VMEM((m, N, N), F32),
        pltpu.VMEM((m, CH, N), F32),
    ]


SEQS = 4
PARTS = 4
VOCAB_HERE = 32
SOURCES = 32
Z, X, Y, C = "batch_0", "batch_1", "head_0", "head_1"
HEAD = (Y, C)
BATCH = (Z, X)
BATCH_HEAD = (Z, X, Y, C)
MESH = pl.DeviceIdType.MESH


def remote(src, dst, send_sem, recv_sem, **place):
    return pltpu.make_async_remote_copy(
        src_ref=src,
        dst_ref=dst,
        send_sem=send_sem,
        recv_sem=recv_sem,
        device_id=place,
        device_id_type=MESH,
    )


def send(src, dst, send_sem, recv_sem, **place):
    copy = remote(src, dst, send_sem, recv_sem, **place)
    copy.start()
    return copy


def arrived(dst, recv_sem):
    pltpu.make_async_remote_copy(
        src_ref=dst,
        dst_ref=dst,
        send_sem=recv_sem,
        recv_sem=recv_sem,
        device_id={C: lax.axis_index(C)},
        device_id_type=MESH,
    ).wait_recv()


def wrap(index, size):
    return lax.rem(index + size, size)


def sent(src, send_sem):
    remote(src, src, send_sem, send_sem, **{C: lax.axis_index(C)}).wait_send()


class Ring:
    def __init__(self, buf, sems, ny):
        self.buf, self.ny = buf, ny
        self.out, self.r_right, self.r_left, self.r_pair = sems
        self.y, self.c = lax.axis_index(Y), lax.axis_index(C)
        long, short = ny // 2, (ny - 1) // 2
        self.steps = [(long, short) if s % 2 == 0 else (short, long) for s in range(PARTS)]
        self.last = long - 1

    def piece(self, owner, core, s):
        size = self.buf.shape[1] // PARTS
        return self.buf.at[owner * 2 + core, pl.ds(s * size, size), :]

    def owner(self, way, k):
        return wrap(self.y - (k + 1), self.ny) if way == 0 else wrap(self.y + (k + 1), self.ny)

    def hop(self, way, k, s):
        piece = self.piece(self.owner(way, k - 1), self.c, s)
        to = wrap(self.y + 1, self.ny) if way == 0 else wrap(self.y - 1, self.ny)
        arrival = (self.r_right, self.r_left)[way].at[k * PARTS + s]
        send(piece, piece, self.out.at[0], arrival, **{Y: to})

    def distance(self, way, k):
        return (-(k + 1) if way == 0 else k + 1) % self.ny

    def to_pair(self, way, k, s):
        piece = self.piece(self.owner(way, k), self.c, s)
        arrival = self.r_pair.at[self.distance(way, k)]
        send(piece, piece, self.out.at[1], arrival, **{C: 1 - self.c})

    def start(self):
        for s in range(PARTS):
            for way in range(2):
                if self.steps[s][way] > 0:
                    self.hop(way, 0, s)
        for s in range(PARTS):
            self.to_pair(0, -1, s)

    def forward(self, k, s):
        for way in range(2):
            if k < self.steps[s][way]:
                owner = self.owner(way, k)
                at = k * PARTS + s
                arrived(self.piece(owner, self.c, s), (self.r_right, self.r_left)[way].at[at])
                if k + 1 < self.steps[s][way]:
                    self.hop(way, k + 1, s)
                self.to_pair(way, k, s)

    def step(self, k):
        for s in range(PARTS):
            self.forward(k, s)

    def wait_pair(self, way, k):
        block = self.buf.at[self.owner(way, k) * 2 + 1 - self.c]
        arrived(block, self.r_pair.at[self.distance(way, k)])

    def owners(self, k):
        return [(0, k), (1, k)] if 2 * (k + 1) < self.ny else [(0, k)]

    def wait_all_pairs(self):
        self.wait_pair(0, -1)
        for k in range(self.last + 1):
            for way, step in self.owners(k):
                self.wait_pair(way, step)

    def drain(self):
        if self.ny > 1:
            sent(self.buf.at[pl.ds(0, self.ny - 1)], self.out.at[0])
        sent(self.buf.at[pl.ds(0, self.ny)], self.out.at[1])


def exchange_head(buf, mine, sems, ny):
    y, c = lax.axis_index(Y), lax.axis_index(C)
    order = sorted(range(1, 2 * ny), key=lambda k: -min(k // 2, ny - k // 2))
    for k in order:
        to = {Y: wrap(y + k // 2, ny), C: lax.rem(c + k % 2, 2)}
        send(buf.at[mine], buf.at[mine], sems.at[0], sems.at[1], **to)


def combine(buf, count):
    parts = [buf[k] for k in range(count)]
    top = functools.reduce(jnp.maximum, [part[0:1] for part in parts])
    total = sum(part[1:2] * jnp.exp(part[0:1] - top) for part in parts)
    target = sum(part[2:3] for part in parts)
    return top, total, target


def put_stats(buf, at, top, total, target):
    buf[at] = jnp.concatenate([top, total, target, jnp.zeros_like(top)], axis=0)


NAMES = (
    "masks", "levels", "tri", "picks", "xs", "acc", "squares", "la", "tt", "tmp", "xh", "xl",
    "kt", "eq", "et", "pq", "rr", "ov", "blocks", "nall", "weight", "cols", "vocab", "state",
    "blank", "lastn", "lastm", "shaped", "hid", "part", "other", "sy", "sp", "tr1", "tr2",
    "tr3", "tr4", "nr1", "nr2", "nr3", "nr4", "c", "d", "v", "a", "b", "z", "x", "p", "g",
    "h", "local", "free", "gain", "rates", "hgain", "fgain", "wanted", "length", "rate",
)


def one_kernel(sizes, *refs):
    (tokens, lengths_in, states, gain_in, mix_weight, rate_in, decay_in, head_in, out_weight,
     final_in, vocab_table, next_in, mixed, new_state, likelihood) = refs[:15]
    r = dict(zip(NAMES, refs[15:]))
    nz, nx, ny = sizes
    heads = 2 * ny
    z, x, y, c = (lax.axis_index(a) for a in BATCH_HEAD)
    me = y * 2 + c
    blocks, nall, cols, hid = r["blocks"], r["nall"], r["cols"], r["hid"]
    local = r["local"]
    gain, rate_t, head_gain, final_gain = r["gain"], r["rates"], r["hgain"], r["fgain"]
    next_token, lengths, rate = r["wanted"], r["length"], r["rate"]
    weight, acc, squares_of = r["weight"], r["acc"], r["squares"]

    own = pltpu.make_async_copy(tokens, blocks.at[me], local.at[0])
    own.start()
    small = []
    for k, (src, dst) in enumerate((
        (gain_in, gain), (rate_in, rate_t), (head_in, head_gain), (final_in, final_gain),
        (next_in, next_token), (lengths_in, lengths), (decay_in, rate),
    )):
        small.append(pltpu.make_async_copy(src, dst, local.at[8 + k]))
        small[-1].start()
    load_weight = pltpu.make_async_copy(mix_weight, weight.at[:, pl.ds(0, 7 * N)], local.at[1])
    load_weight.start()
    load_state = pltpu.make_async_copy(states, r["state"], local.at[2])
    load_state.start()
    band = N // nx
    rows_here = pl.ds(pl.multiple_of(x * band, band), band)
    own_cols = pltpu.make_async_copy(
        out_weight.at[rows_here, pl.ds(pl.multiple_of(me * N, N), N)],
        cols.at[me, rows_here, :],
        local.at[3],
    )
    own_cols.start()
    quarter = heads * N // 8
    vocab_copies = []

    def vocab_piece(half, q):
        start = pl.multiple_of(half * (4 * quarter) + q * quarter, N)
        rows = pl.ds(pl.multiple_of(q * 2 * VOCAB_HERE + c * VOCAB_HERE, VOCAB_HERE), VOCAB_HERE)
        return vocab_table.at[:, pl.ds(start, quarter)], r["vocab"].at[rows, :]

    for q in range(4):
        src, dst = vocab_piece(c, q)
        copy = pltpu.make_async_copy(src, dst, local.at[4 + q])
        copy.start()
        vocab_copies.append(copy)
    if nz * nx < SOURCES:
        hid[...] = jnp.zeros_like(hid)

    barrier = pltpu.get_barrier_semaphore()
    near = [{C: 1 - c}]
    for axis, size, at in ((Y, ny, y), (Z, nz, z), (X, nx, x)):
        if size > 1:
            near += [{axis: wrap(at + 1, size)}, {axis: wrap(at - 1, size)}]
    for place in near:
        pl.semaphore_signal(barrier, inc=1, device_id=place, device_id_type=MESH)
    own.wait()
    pl.semaphore_wait(barrier, len(near))

    ring = Ring(blocks, [r[f"tr{k}"] for k in range(1, 5)], ny)
    ring.start()
    last_sends = []

    def shared(ref, sems):
        arrived(ref, sems.at[1])
        last_sends.append((ref, sems.at[0]))

    for q in range(4):
        src, dst = vocab_piece(1 - c, q)
        send(src, dst, r["v"].at[0], r["v"].at[1], **{C: 1 - c})

    pending = []
    free = r["free"]
    for slot, (axis, size, at) in enumerate(((X, nx, x), (Z, nz, z))):
        for _ in range(size - 1):
            def signal(slot=slot, axis=axis, size=size, at=at):
                pl.semaphore_signal(
                    free.at[slot], inc=1, device_id={axis: wrap(at + 1, size)}, device_id_type=MESH
                )

            def await_signal(slot=slot):
                pl.semaphore_wait(free.at[slot], 1)

            pending += [signal, await_signal]

    def plane_step():
        if pending:
            pending.pop(0)()

    def plane_next():
        plane_step()
        plane_step()

    if pending:
        plane_step()
    fill_tables(r["masks"], r["levels"], r["tri"], r["picks"])
    for copy in small:
        copy.wait()
    place_rates(rate_t, weight, r["blank"])
    load_weight.wait()

    def ready(arrivals):
        for way, k in arrivals:
            ring.wait_pair(way, k)
        owners = [ring.owner(way, k) for way, k in arrivals]
        fresh = arrivals[0][1] < 0
        widen(owners, fresh, blocks, gain, r["xs"], squares_of)
        return owners, fresh

    def take(owners, fresh, quarters):
        for quarter in quarters:
            absorb(owners, fresh, quarter, weight, r["xs"], acc)

    for k in range(ring.last + 1):
        ring.forward(k, 0)
        if k:
            found = ready([(0, -1)] if k == 1 else ring.owners(k - 2))
        ring.forward(k, 1)
        if k:
            take(*found, (0,))
        plane_next()
        ring.forward(k, 2)
        if k:
            take(*found, (1,))
        ring.forward(k, 3)
        if k:
            take(*found, (2, 3))
        plane_next()

    for k in range(1, heads):
        py, pc = wrap(y + k // 2, ny), lax.rem(c + k % 2, 2)
        to = pl.multiple_of((py * 2 + pc) * N, N)
        send(out_weight.at[rows_here, pl.ds(to, N)], cols.at[me, rows_here, :], r["c"].at[0],
             r["c"].at[1], **{Y: py, C: pc})
    for k in range(max(ring.last - 1, 0), ring.last + 1):
        take(*ready(ring.owners(k)), range(4))
    plane_next()
    for s in range(SEQS):
        sequence_inputs(
            s, lengths[s], rate[0, 0], heads, acc, squares_of, r["masks"], r["tri"], r["picks"],
            r["la"], r["tt"], r["tmp"], r["xh"], r["xl"], r["kt"], r["eq"], r["et"],
        )
    plane_next()
    ids = range(SEQS * NC)
    invert(ids, 2, 5, r["levels"], r["la"], r["tt"], r["tmp"])
    plane_next()
    own_cols.wait()
    shared(cols.at[pl.ds(0, heads - 1), rows_here, :], r["c"])
    bands = cols.at[:, rows_here, :]
    for dx in range(1, nx):
        send(bands, bands, r["d"].at[0], r["d"].at[1], **{X: wrap(x + dx, nx)})
    invert(ids, 5, LEVELS, r["levels"], r["la"], r["tt"], r["tmp"])
    plane_next()
    for n in ids:
        chunk_maps(
            n, r["tt"], r["xh"], r["xl"], r["kt"], r["eq"], r["et"], r["pq"], r["rr"], r["ov"]
        )
    load_state.wait()
    plane_next()
    run_chain(
        range(SEQS), r["state"], new_state, nall.at[me], head_gain, r["pq"], r["rr"], r["ov"]
    )

    position = lax.broadcasted_iota(jnp.int32, (N, N), 0)

    def last_rows(ref):
        rows = []
        for s in range(SEQS):
            wide = ref[me, s * N : (s + 1) * N, :].astype(F32)
            kept = jnp.where(position == lengths[s] - 1, wide, 0.0)
            rows.append(jnp.sum(kept, axis=0, keepdims=True))
        return jnp.concatenate(rows, axis=0)

    lastn, lastm = r["lastn"], r["lastm"]
    lastn[me] = last_rows(nall)
    exchange_head(lastn, me, r["a"], ny)
    bulk = Ring(nall, [r[f"nr{k}"] for k in range(1, 5)], ny)
    residual = last_rows(blocks)
    if nx > 1:
        shared(cols.at[:, pl.ds(0, (nx - 1) * band), :], r["d"])
    shared(lastn.at[pl.ds(0, heads - 1)], r["a"])
    wide = jnp.concatenate([lastn[b].astype(BF) for b in range(heads)], axis=1)
    every_col = jnp.concatenate([cols[b] for b in range(heads)], axis=0)
    lastm[me] = (residual + dot(wide, every_col)).astype(BF).astype(F32)
    exchange_head(lastm, me, r["b"], ny)
    bulk.start()
    late = list(range(ring.last + 1))

    def bulk_step():
        if late:
            bulk.step(late.pop(0))

    while pending:
        plane_step()
    shared(lastm.at[pl.ds(0, heads - 1)], r["b"])
    squares = sum(lastm[b] * lastm[b] for b in range(heads))
    factor = lax.rsqrt(jnp.sum(squares, axis=1, keepdims=True) / (heads * N) + ROW_EPSILON)
    per = heads // 8
    shaped = r["shaped"]
    for q in range(4):
        for k in range(per):
            b = c * (heads // 2) + q * per + k
            shaped[q * SEQS : (q + 1) * SEQS, k * N : (k + 1) * N] = (
                lastm[b] * factor * final_gain[pl.ds(b, 1), :]
            )
    slot = x * nz + z
    hid[slot] = shaped[...].astype(BF)
    def cell(px, pz):
        return hid.at[px * nz + pz]

    def to_row(pz):
        for dx in range(1, nx):
            send(cell(x, pz), cell(x, pz), r["x"].at[0], r["x"].at[1], **{X: wrap(x + dx, nx)})

    for k in sorted(range(1, nz), key=lambda k: -min(k, nz - k)):
        send(cell(x, z), cell(x, z), r["z"].at[0], r["z"].at[k], **{Z: wrap(z + k, nz)})
    to_row(z)
    bulk_step()
    for k in sorted(range(1, nz), key=lambda k: min(k, nz - k)):
        pz = wrap(z - k, nz)
        arrived(cell(x, pz), r["z"].at[k])
        to_row(pz)
    bulk_step()
    for q in range(4):
        vocab_copies[q].wait()
    shared(r["vocab"].at[pl.ds(0, 4 * VOCAB_HERE), :], r["v"])
    lane = lax.broadcasted_iota(jnp.int32, (N, N), 1)
    rank = lax.broadcasted_iota(jnp.int32, (N, N), 0)
    source = ((lane // 4) % 4) * 8 + lane // 16
    order = (lax.rem(source, nz) * nx + source // nz) * SEQS + lane % 4
    permute = ((order == rank) & (source < nz * nx)).astype(F32)
    wanted = jnp.broadcast_to(next_token[...].astype(F32), (8, N))
    wanted = jnp.dot(wanted, permute, precision=HI, preferred_element_type=F32)[0:1]
    wanted = (wanted + 0.5).astype(jnp.int32)
    if nx > 1:
        shared(hid.at[pl.ds(0, (nx - 1) * nz)], r["x"])
    if nz > 1:
        last_sends.append((hid.at[pl.ds(0, nz - 1)], r["z"].at[0]))

    everyone = jnp.concatenate([hid[k] for k in range(SOURCES)], axis=0)
    product = dot_nt(r["vocab"][...], everyone)
    height = 2 * VOCAB_HERE
    quarter_of = (lane[:height] % 16) // 4
    packed = jnp.zeros((height, N), F32)
    for k in range(4):
        mine = jnp.zeros((height, N), F32)
        for q in range(4):
            block = product[q * height : (q + 1) * height, k * N : (k + 1) * N]
            mine = mine + jnp.where(quarter_of == q, block, 0.0)
        mine = mine + pltpu.roll(mine, N - 4, 1)
        mine = mine + pltpu.roll(mine, N - 8, 1)
        if k:
            mine = pltpu.roll(mine, 4 * k, 1)
        packed = packed + jnp.where(quarter_of == k, mine, 0.0)
    part, other = r["part"], r["other"]
    part[0] = packed[:VOCAB_HERE]
    part[1] = packed[VOCAB_HERE:]
    send(part.at[1 - c], other, r["p"].at[0], r["p"].at[1], **{C: 1 - c})
    shared(other, r["p"])
    logits = part[c] + other[...]
    vocab_ids = (((z * nx + x) * ny + y) * 2 + c) * VOCAB_HERE + rank[:VOCAB_HERE]
    top = jnp.max(logits, axis=0, keepdims=True)
    total = jnp.sum(jnp.exp(logits - top), axis=0, keepdims=True)
    target = jnp.sum(jnp.where(vocab_ids == wanted, logits, 0.0), axis=0, keepdims=True)
    sy, sp = r["sy"], r["sp"]
    put_stats(sy, me, top, total, target)
    exchange_head(sy, me, r["g"], ny)
    bulk_step()
    shared(sy.at[pl.ds(0, heads - 1)], r["g"])
    put_stats(sp, slot, *combine(sy, heads))
    far = sorted(
        (k for k in range(1, nz * nx)),
        key=lambda k: -min(k % nz, nz - k % nz) - min(k // nz, nx - k // nz),
    )
    for k in far:
        to = {Z: wrap(z + k % nz, nz), X: wrap(x + k // nz, nx)}
        send(sp.at[slot], sp.at[slot], r["h"].at[0], r["h"].at[1], **to)
    while late:
        bulk_step()
    bulk.wait_all_pairs()

    def mix(s, carry):
        rows = pl.ds(pl.multiple_of(s * N, N), N)
        wide = jnp.concatenate([nall[b, rows, :] for b in range(heads)], axis=1)
        every = jnp.concatenate([cols[b] for b in range(heads)], axis=0)
        mixed[rows, :] = (blocks[me, rows, :].astype(F32) + dot(wide, every)).astype(BF)
        return carry

    lax.fori_loop(0, SEQS, mix, 0)
    ring.drain()
    bulk.drain()
    for src, sem in last_sends:
        sent(src, sem)
    last_sends.clear()
    shared(sp.at[pl.ds(0, nz * nx - 1)], r["h"])
    top, total, target = combine(sp, nz * nx)
    result = jnp.broadcast_to(target - (top + jnp.log(total)), (8, N))
    likelihood[...] = lax.dot_general(
        result, permute, (((1,), (1,)), ((), ())), precision=HI, preferred_element_type=F32
    )[0:1]
    for src, sem in last_sends:
        sent(src, sem)


def deliver_kernel(*refs):
    sems = refs[-1]
    copies = [pltpu.make_async_copy(refs[k], refs[3 + k], sems.at[k]) for k in range(3)]
    for copy in copies:
        copy.start()
    for copy in copies:
        copy.wait()


def deliver(*arrays):
    return pl.pallas_call(
        deliver_kernel,
        out_shape=tuple(jax.ShapeDtypeStruct(a.shape, a.dtype) for a in arrays),
        in_specs=[pl.BlockSpec(memory_space=pltpu.VMEM)] * 3,
        out_specs=(pl.BlockSpec(memory_space=pl.ANY),) * 3,
        scratch_shapes=[pltpu.SemaphoreType.DMA((3,))],
    )(*arrays)


def on_device(sizes, tokens, lengths, states, norm_gain, mix_weight, rate_weight, decay_rate,
              head_gain, out_weight, final_gain, vocab_table, next_token):
    nz, nx, ny = sizes
    heads = 2 * ny
    rows = SEQS * N
    everyone = next_token.shape[0]
    vmem = pl.BlockSpec(memory_space=pltpu.VMEM)
    hbm = pl.BlockSpec(memory_space=pltpu.HBM)
    dma = lambda n: pltpu.SemaphoreType.DMA((max(n, 1),))
    scratch = mixer_scratch(SEQS, heads, mix_weight.shape[1]) + [
        pltpu.VMEM((heads, rows, N), BF),
        pltpu.VMEM((heads, rows, N), BF),
        pltpu.VMEM((heads * N, 8 * N), BF),
        pltpu.VMEM((heads, N, N), BF),
        pltpu.VMEM((8 * VOCAB_HERE, heads * N // 8), BF),
        pltpu.VMEM((SEQS, N, N), F32),
        pltpu.VMEM((N, N), F32),
        pltpu.VMEM((heads, SEQS, N), F32),
        pltpu.VMEM((heads, SEQS, N), F32),
        pltpu.VMEM((4 * SEQS, heads * N // 8), F32),
        pltpu.VMEM((SOURCES, 4 * SEQS, heads * N // 8), BF),
        pltpu.VMEM((2, VOCAB_HERE, N), F32),
        pltpu.VMEM((VOCAB_HERE, N), F32),
        pltpu.VMEM((heads, 4, N), F32),
        pltpu.VMEM((nz * nx, 4, N), F32),
    ]
    hops = PARTS * max(ny // 2, 1)
    scratch += [dma(2), dma(hops), dma(hops), dma(ny)] * 2
    scratch += [dma(2)] * 5 + [dma(nz)] + [dma(2)] * 4
    scratch += [dma(15), pltpu.SemaphoreType.REGULAR((2,))]
    scratch += [
        pltpu.VMEM((heads, N), F32),
        pltpu.VMEM((4, heads * N), BF),
        pltpu.VMEM((1, N), F32),
        pltpu.VMEM((heads, N), F32),
        pltpu.VMEM((1, N), jnp.int32),
        pltpu.SMEM((SEQS,), jnp.int32),
        pltpu.SMEM((1, 1), F32),
    ]
    wanted = next_token.reshape(1, everyone)
    if everyone < N:
        wanted = jnp.pad(wanted, ((0, 0), (0, N - everyone)))
    mixed, new_state, likelihood = pl.pallas_call(
        functools.partial(one_kernel, sizes),
        out_shape=(
            jax.ShapeDtypeStruct((rows, N), BF),
            jax.ShapeDtypeStruct((SEQS, N, N), F32),
            jax.ShapeDtypeStruct((1, N), F32),
        ),
        in_specs=[hbm] * 12,
        out_specs=(vmem, vmem, vmem),
        scratch_shapes=scratch,
        compiler_params=pltpu.CompilerParams(
            collective_id=0, has_side_effects=True, vmem_limit_bytes=63 * 1024 * 1024
        ),
    )(
        tokens,
        lengths,
        states[:, 0],
        norm_gain.reshape(heads, N),
        mix_weight,
        rate_weight.T,
        decay_rate.reshape(1, 1),
        head_gain.reshape(1, N),
        out_weight,
        final_gain.reshape(heads, N),
        vocab_table,
        wanted,
    )
    mixed, new_state, likelihood = deliver(mixed, new_state, likelihood)
    return mixed, new_state[:, None], likelihood[0, :everyone]


def build(torus):
    sizes = (torus.shape[Z], torus.shape[X], torus.shape[Y])
    placed = (
        P(BATCH, HEAD),
        P(BATCH),
        P(BATCH, HEAD, None, None),
        P(),
        P(None, HEAD),
        P(None, HEAD),
        P(HEAD),
        P(),
        P(HEAD, None),
        P(),
        P(BATCH_HEAD, None),
        P(),
    )
    return jax.shard_map(
        functools.partial(on_device, sizes),
        mesh=torus,
        in_specs=placed,
        out_specs=(P(BATCH, HEAD), P(BATCH, HEAD, None, None), P()),
        check_vma=False,
    )


def solution(mesh):
    torus = Mesh(mesh.devices.reshape(8, 4, 8, 2), BATCH_HEAD)
    return build(torus)
```
